32 devices in a mesh: rows: 8 (over y, x, core), model: 4 (over z).
Axes of the slice: x: 2, y: 2, z: 4, core: 2. Of those that a mesh axis runs over, the one named last changes fastest.
Arguments:
- one_query: float32 [5120, 5120], P('rows', 'model'), may hold values from -0.125 to 0.125
- other_query: float32 [5120, 5120], P('rows', 'model'), may hold values from -0.078125 to 0.078125
- one_key: float32 [5120, 5120], P('rows', 'model'), may hold values from -0.125 to 0.125
- other_key: float32 [5120, 5120], P('rows', 'model'), may hold values from -0.078125 to 0.078125
- one_value: float32 [5120, 5120], P('rows', 'model'), may hold values from -0.125 to 0.125
- other_value: float32 [5120, 5120], P('rows', 'model'), may hold values from -0.078125 to 0.078125
- mix_share: float32 [5120], P('rows'), may hold values from 0.2 to 0.8
- norm_gain: float32 [5120], P('rows'), may hold values from 0.25 to 1.75
Outputs:
- final_query: bfloat16 [5120, 5120], P(None, 'model')
- final_key: bfloat16 [5120, 5120], P(None, 'model')
- final_value: bfloat16 [5120, 5120], P(None, 'model')
- factor_query: float32 [5120], P('model')
- factor_key: float32 [5120], P('model')
- factor_value: float32 [5120], P('model')
The draws below stay inside these ranges and needn't reach their ends.
All inputs are finite; a program needn't handle non-finite values. Where the reference program divides by a largest or mean magnitude, that divisor is 1e-20 or more.
Results may differ from the reference program's by a relative error of at most 0.001.
Values may be sent and summed in bfloat16 or wider, within the bound.
A program may use at most 192 MiB of HBM per device.

```python
import jax
import jax.numpy as jnp

D_MODEL = 5120
Q_DIM = 5120
KV_DIM = 5120


def raised(array, stream_key, source, target, blocks, factor):
    def block_of(position):
        return (jnp.arange(array.shape[position]) // (array.shape[position] // blocks)).reshape((-1,) + (1,) * (array.ndim - 1 - position))

    near = jax.random.permutation(stream_key, blocks)[block_of(target)]
    far = (block_of(target) + blocks // 2) % blocks
    return jnp.where((block_of(source) == near) | (block_of(source) == far), factor * array, array)


def level_of(rng, dims, pieces, least, high):
    gain = 1.0
    for position, blocks in pieces:
        draws = jax.random.uniform(jax.random.fold_in(jax.random.fold_in(rng, 6), position), (blocks,), jnp.float32, least / len(pieces), high / len(pieces))
        gain = gain * jnp.repeat(jnp.exp(draws), dims[position] // blocks).reshape((-1,) + (1,) * (len(dims) - 1 - position))
    return gain


def normal_values(rng, dims, spread, bound, split=(), kind=jnp.bfloat16):
    level = level_of(rng, dims, split, -0.22, 0.18) if split else 1.0
    result = jax.random.normal(rng, dims, jnp.float32) * spread * level
    return jnp.minimum(jnp.maximum(result, -bound), bound).astype(kind)


def noise_with(rng, dims, deviation, most, split, heavy, kind=jnp.bfloat16):
    entries = deviation * jax.random.normal(rng, dims, jnp.float32)
    if split:
        entries = entries * level_of(rng, dims, split, -0.22, 0.18)
    return jnp.clip(raised(entries, jax.random.fold_in(rng, 3), *heavy), -most, most).astype(kind)


def setup_inputs(seed: int = 0) -> dict:
    arg_keys = jax.random.split(jax.random.key(seed), 9)
    return {
        "one_query": noise_with(arg_keys[0], (D_MODEL, Q_DIM), D_MODEL ** -0.5, 0.125, ((0, 8), (1, 4)), (0, 1, 8, 2.0), jnp.float32),
        "other_query": normal_values(arg_keys[1], (D_MODEL, Q_DIM), D_MODEL ** -0.5, 0.078125, ((0, 8), (1, 4)), jnp.float32),
        "one_key": noise_with(arg_keys[2], (D_MODEL, KV_DIM), D_MODEL ** -0.5, 0.125, ((0, 8), (1, 4)), (0, 1, 8, 2.0), jnp.float32),
        "other_key": normal_values(arg_keys[3], (D_MODEL, KV_DIM), D_MODEL ** -0.5, 0.078125, ((0, 8), (1, 4)), jnp.float32),
        "one_value": noise_with(arg_keys[4], (D_MODEL, KV_DIM), D_MODEL ** -0.5, 0.125, ((0, 8), (1, 4)), (0, 1, 8, 2.0), jnp.float32),
        "other_value": normal_values(arg_keys[5], (D_MODEL, KV_DIM), D_MODEL ** -0.5, 0.078125, ((0, 8), (1, 4)), jnp.float32),
        "mix_share": jnp.clip(0.2 + 0.6 * jax.random.uniform(arg_keys[6], (D_MODEL,), jnp.float32) ** level_of(arg_keys[6], (D_MODEL,), ((0, 8),), -0.2, 0.2), 0.2, 0.8),
        "norm_gain": jnp.clip(1.0 + 0.15 * jax.random.normal(arg_keys[7], (D_MODEL,), jnp.float32), 0.25, 1.75),
    }


def reference(one_query, other_query, one_key, other_key, one_value, other_value, mix_share, norm_gain):
    result_query = mix_share[:, None] * one_query + (1.0 - mix_share[:, None]) * other_query
    result_key = mix_share[:, None] * one_key + (1.0 - mix_share[:, None]) * other_key
    result_value = mix_share[:, None] * one_value + (1.0 - mix_share[:, None]) * other_value
    result_gained_query = result_query * norm_gain[:, None]
    result_gained_key = result_key * norm_gain[:, None]
    result_gained_value = result_value * norm_gain[:, None]
    factor_query = jnp.max(jnp.abs(result_gained_query), axis=0)
    final_query = (result_gained_query / factor_query).astype(jnp.bfloat16)
    factor_key = jnp.max(jnp.abs(result_gained_key), axis=0)
    final_key = (result_gained_key / factor_key).astype(jnp.bfloat16)
    factor_value = jnp.max(jnp.abs(result_gained_value), axis=0)
    final_value = (result_gained_value / factor_value).astype(jnp.bfloat16)
    return final_query, final_key, final_value, factor_query, factor_key, factor_value
```

```python
import functools

import jax
import jax.numpy as jnp
from jax import lax
from jax.experimental import pallas as pl
from jax.experimental.pallas import tpu as pltpu
from jax.sharding import PartitionSpec as P

MESH = pl.DeviceIdType.MESH
LANES = 128
OWN_X, OWN_Y, OWN_S, DIAG, X_S, Y_S, D_S = range(7)


def gathered_by_collectives(one_query, other_query, one_key, other_key, one_value, other_value, mix_share, norm_gain):
    share, gain = mix_share[:, None], norm_gain[:, None]
    gained = [
        (share * one + (1.0 - share) * other) * gain
        for one, other in ((one_query, other_query), (one_key, other_key), (one_value, other_value))
    ]
    factors = lax.pmax(tuple(jnp.max(jnp.abs(g), axis=0) for g in gained), "rows")
    narrow = [(g / f).astype(jnp.bfloat16) for g, f in zip(gained, factors)]
    return (*(lax.all_gather(w, "rows", axis=0, tiled=True) for w in narrow), *factors)


def opposite(me, d):
    core, east, north = lax.rem(me, 2), lax.rem(me // 2, 2), me // 4
    return (
        lax.rem(north + d // 4, 2) * 4
        + lax.rem(east + (d // 2) % 2, 2) * 2
        + lax.rem(core + d % 2, 2)
    )


def late_chunks(chunks, m):
    return (0, 1, chunks // 2)[m]


def late_slot(chunks, m, k):
    half = chunks // 2
    if m == 2:
        return k % half
    if m == 1 and k in (0, chunks - 1):
        return half
    return None


def kernel(chunks, share, gain, *refs):
    args, factors = refs[0:6], refs[6]
    outs, late = [refs[7].at[m] for m in range(3)], refs[8]
    (held, wide_one, wide_other, box_first, box_rest,
     load_sem, send_sem, bulk_sem, x_sem, y_sem, d_sem, box_sem, late_sem) = refs[9:]
    rows, columns = args[0].shape
    height = rows // chunks
    half = chunks // 2
    tiles = columns // LANES

    me = lax.axis_index("rows")
    core = lax.rem(me, 2)

    def peer(d):
        return opposite(me, d)

    sibling, at_x, at_y, at_d = peer(1), peer(2), peer(4), peer(6)

    loads = [pltpu.make_async_copy(args[i], held.at[i], load_sem.at[i]) for i in range(6)]
    for load in loads:
        load.start()

    barrier = pltpu.get_barrier_semaphore()
    for d in range(1, 8):
        pl.semaphore_signal(barrier, inc=1, device_id={"rows": peer(d)}, device_id_type=MESH)

    for j in range(rows // LANES):
        s = jnp.broadcast_to(share[j * LANES:(j + 1) * LANES][None], (LANES, LANES)).T
        g = jnp.broadcast_to(gain[j * LANES:(j + 1) * LANES][None], (LANES, LANES)).T
        wide_one[j * LANES:(j + 1) * LANES, :] = s * g
        wide_other[j * LANES:(j + 1) * LANES, :] = (1.0 - s) * g

    def mix(m):
        loads[2 * m].wait()
        loads[2 * m + 1].wait()

        def body(i, top):
            at = pl.ds(pl.multiple_of(i * 8, 8), 8)
            a = jnp.concatenate([wide_one[at, :]] * tiles, axis=1)
            b = jnp.concatenate([wide_other[at, :]] * tiles, axis=1)
            mixed = a * held[2 * m, at, :] + b * held[2 * m + 1, at, :]
            held[2 * m, at, :] = mixed
            return jnp.maximum(top, jnp.abs(mixed))

        top = lax.fori_loop(0, rows // 8, body, jnp.zeros((8, columns), jnp.float32), unroll=4)
        return jnp.max(top, axis=0, keepdims=True)

    def exchange(box, which):
        return [
            pltpu.make_async_remote_copy(
                box.at[me], box.at[me], box_sem.at[2 * which], box_sem.at[2 * which + 1],
                device_id={"rows": peer(d)}, device_id_type=MESH,
            )
            for d in range(1, 8)
        ]

    def exchanged(box, which):
        return pltpu.make_async_remote_copy(
            box.at[pl.ds(0, 7)], box.at[pl.ds(0, 7)], box_sem.at[2 * which], box_sem.at[2 * which + 1],
            device_id={"rows": sibling}, device_id_type=MESH,
        )

    def piece(m, owner, k):
        return outs[m].at[pl.ds(pl.multiple_of(owner * rows + k * height, 16), height), :]

    def copy(m, owner, k, stream, target):
        ref = piece(m, owner, k)
        arrive = {OWN_X: x_sem, OWN_Y: y_sem, DIAG: d_sem}.get(stream)
        arrive = bulk_sem.at[m, stream] if arrive is None else arrive.at[m, k]
        return pltpu.make_async_remote_copy(
            ref, ref, send_sem.at[m, stream], arrive,
            device_id={"rows": target}, device_id_type=MESH,
        )

    def whole(m, stream):
        size = rows - height * late_chunks(chunks, m) if stream in (DIAG, D_S) else rows
        ref = outs[m].at[pl.ds(0, size), :]
        return pltpu.make_async_remote_copy(
            ref, ref, send_sem.at[m, stream], bulk_sem.at[m, stream],
            device_id={"rows": sibling}, device_id_type=MESH,
        )

    def narrow(m, k, inverse):
        def body(i, _):
            at = pl.multiple_of(k * height + i * 16, 16)
            small = (held[2 * m, pl.ds(at, 16), :] * inverse).astype(jnp.bfloat16)
            outs[m][pl.ds(pl.multiple_of(me * rows + at, 16), 16), :] = small
            return 0

        lax.fori_loop(0, height // 16, body, 0, unroll=True)

    def send_own(m, k):
        copy(m, me, k, OWN_X, at_x).start()
        copy(m, me, k, OWN_Y, at_y).start()
        copy(m, me, k, OWN_S, sibling).start()

    box_first[me] = mix(0)
    pl.semaphore_wait(barrier, 7)
    for c in exchange(box_first, 0):
        c.start()
    exchanged(box_first, 0).wait_recv()
    factor = jnp.max(box_first[...], axis=0)
    factors[0] = factor
    inverse = 1.0 / factor
    for k in range(chunks):
        narrow(0, k, inverse)
        if 1 <= k <= half:
            send_own(0, k - 1)

    box_rest[me, 0:1] = mix(1)
    box_rest[me, 1:2] = mix(2)
    for c in exchange(box_rest, 1):
        c.start()
    for k in range(half, chunks):
        send_own(0, k)
    exchanged(box_rest, 1).wait_recv()
    both = jnp.max(box_rest[...], axis=0)
    for m in (1, 2):
        factor = both[m - 1:m]
        factors[m] = factor
        inverse = 1.0 / factor
        for k in range(chunks):
            narrow(m, k, inverse)
            if k:
                send_own(m, k - 1)
        send_own(m, chunks - 1)

    def put_aside(m, owner, k, slot):
        return pltpu.make_async_copy(
            piece(m, owner, k), late.at[pl.ds(slot * height, height), :], late_sem
        )

    def unless_late(m, k, then, otherwise):
        via = k // half
        slot = late_slot(chunks, m, k)
        if slot is None:
            then()
        else:
            pl.when(core == via)(then)
            pl.when(core != via)(lambda: otherwise(slot))

    def relay(m, k, owner, target):
        unless_late(
            m, k,
            copy(m, owner, k, DIAG, target).start,
            lambda slot: put_aside(m, owner, k, slot).start(),
        )

    def relayed(m, k):
        def then():
            copy(m, at_d, k, DIAG, at_y).wait_recv()
            copy(m, at_d, k, D_S, sibling).start()

        if late_slot(chunks, m, k) is None:
            then()
        else:
            pl.when(core == k // half)(then)

    for m in range(3):
        for k in range(chunks):
            copy(m, at_x, k, OWN_X, at_x).wait_recv()
            copy(m, at_x, k, X_S, sibling).start()
            if k < half:
                relay(m, k, at_x, at_y)
            copy(m, at_y, k, OWN_Y, at_y).wait_recv()
            copy(m, at_y, k, Y_S, sibling).start()
            if k >= half:
                relay(m, k, at_y, at_x)
    for m in range(3):
        for k in range(half):
            for part in (k, k + half):
                relayed(m, part)

    for m in range(3):
        for stream in (OWN_S, X_S, Y_S, D_S):
            whole(m, stream).wait_recv()
    for m in range(3):
        for stream in range(7):
            whole(m, stream).wait_send()
    pltpu.make_async_copy(outs[0].at[pl.ds(0, late.shape[0]), :], late, late_sem).wait()
    exchanged(box_first, 0).wait_send()
    exchanged(box_rest, 1).wait_send()


def settle(chunks, factors, gathered, *refs):
    targets, sems = refs[:6], refs[6]
    rows = gathered.shape[1] // 8
    height = rows // chunks
    me = lax.axis_index("rows")
    copies = []
    for d in range(8):
        owner = opposite(me, d)
        core = lax.rem(owner, 2)
        for m in range(3):
            late = height * late_chunks(chunks, m) if d >= 6 else 0
            at = pl.multiple_of(owner * rows + core * late, 16)
            copies.append(
                pltpu.make_async_copy(
                    gathered.at[m, pl.ds(at, rows - late), :],
                    targets[m].at[pl.ds(at, rows - late), :],
                    sems.at[m, d],
                )
            )
    for c in copies:
        c.start()
    for m in range(3):
        targets[3 + m][...] = factors[m, 0]
    for c in copies:
        c.wait()


def finish(chunks, mine, other, key, value, out_key, out_value, sems):
    rows = value.shape[0] // 8
    height, half = rows // chunks, chunks // 2
    me = lax.axis_index("rows")
    copies = []
    for d, late in ((6, mine), (7, other)):
        owner = opposite(me, d)
        core = lax.rem(owner, 2)
        at = pl.multiple_of(owner * rows + (1 - core) * half * height, 16)
        copies.append(
            pltpu.make_async_copy(
                late.at[pl.ds(0, half * height), :],
                out_value.at[pl.ds(at, half * height), :],
                sems.at[0, d - 6],
            )
        )
        at = pl.multiple_of(owner * rows + (1 - core) * (chunks - 1) * height, 16)
        copies.append(
            pltpu.make_async_copy(
                late.at[pl.ds(half * height, height), :],
                out_key.at[pl.ds(at, height), :],
                sems.at[1, d - 6],
            )
        )
    for c in copies:
        c.start()
    for c in copies:
        c.wait()


def gathered_by_kernel(*arrays):
    *weights, mix_share, norm_gain = arrays
    rows, columns = weights[0].shape
    chunks = 8
    late_rows = rows // chunks * sum(late_chunks(chunks, m) for m in range(3))
    vmem, hbm = pl.BlockSpec(memory_space=pltpu.VMEM), pl.BlockSpec(memory_space=pltpu.HBM)
    anywhere = pl.BlockSpec(memory_space=pl.ANY)
    dma = pltpu.SemaphoreType.DMA
    results = pl.pallas_call(
        functools.partial(kernel, chunks),
        out_shape=[
            pltpu.VMEM((3, 1, columns), jnp.float32),
            pltpu.VMEM((3, 8 * rows, columns), jnp.bfloat16),
            pltpu.VMEM((late_rows, columns), jnp.bfloat16),
        ],
        in_specs=[vmem] * 2 + [hbm] * 6,
        out_specs=[vmem] * 3,
        scratch_shapes=[
            pltpu.VMEM((6, rows, columns), jnp.float32),
            pltpu.VMEM((rows, LANES), jnp.float32),
            pltpu.VMEM((rows, LANES), jnp.float32),
            pltpu.VMEM((8, 1, columns), jnp.float32),
            pltpu.VMEM((8, 2, columns), jnp.float32),
            dma((6,)),
            dma((3, 7)),
            dma((3, 7)),
            dma((3, chunks)),
            dma((3, chunks)),
            dma((3, chunks)),
            dma((4,)),
            dma(()),
        ],
        compiler_params=pltpu.CompilerParams(
            collective_id=0, has_side_effects=True, vmem_limit_bytes=21 * 2**20
        ),
    )(mix_share, norm_gain, *weights)
    factors, gathered, late = [pltpu.with_memory_space_constraint(r, pltpu.VMEM) for r in results]
    whole = jax.ShapeDtypeStruct((8 * rows, columns), jnp.bfloat16)
    mine = lax.ppermute(late, "rows", [(i, i ^ (2, 4)[i % 2]) for i in range(8)])
    query, key, value, *factors = pl.pallas_call(
        functools.partial(settle, chunks),
        out_shape=[whole] * 3 + [jax.ShapeDtypeStruct((columns,), jnp.float32)] * 3,
        in_specs=[vmem] * 2,
        out_specs=[anywhere] * 3 + [vmem] * 3,
        scratch_shapes=[dma((3, 8))],
        cost_estimate=pl.CostEstimate(flops=0, bytes_accessed=48 * rows * columns, transcendentals=0),
        compiler_params=pltpu.CompilerParams(vmem_limit_bytes=2**20),
    )(factors, gathered)
    mine, key, value = lax.optimization_barrier((mine, key, value))
    other = lax.ppermute(mine, "rows", [(i, i ^ 1) for i in range(8)])
    key, value = pl.pallas_call(
        functools.partial(finish, chunks),
        out_shape=[whole] * 2,
        in_specs=[vmem] * 2 + [anywhere] * 2,
        out_specs=[anywhere] * 2,
        scratch_shapes=[dma((2, 2))],
        input_output_aliases={2: 0, 3: 1},
        compiler_params=pltpu.CompilerParams(vmem_limit_bytes=2**20),
    )(mine, other, key, value)
    return query, key, value, *factors


def solution(mesh):
    placed = (P("rows", "model"),) * 6 + (P("rows"),) * 2
    local = gathered_by_kernel if mesh.shape["rows"] == 8 else gathered_by_collectives
    return jax.shard_map(
        local,
        mesh=mesh,
        in_specs=placed,
        out_specs=(P(None, "model"),) * 3 + (P("model"),) * 3,
        check_vma=False,
    )
```

```python
import functools

import jax
import jax.numpy as jnp
from jax import lax
from jax.experimental import pallas as pl
from jax.experimental.pallas import tpu as pltpu
from jax.sharding import PartitionSpec as P

MESH = pl.DeviceIdType.MESH
LANES = 128
OWN_X, OWN_Y, OWN_S, DIAG, X_S, Y_S, D_S = range(7)


def gathered_by_collectives(one_query, other_query, one_key, other_key, one_value, other_value, mix_share, norm_gain):
    share, gain = mix_share[:, None], norm_gain[:, None]
    gained = [
        (share * one + (1.0 - share) * other) * gain
        for one, other in ((one_query, other_query), (one_key, other_key), (one_value, other_value))
    ]
    factors = lax.pmax(tuple(jnp.max(jnp.abs(g), axis=0) for g in gained), "rows")
    narrow = [(g / f).astype(jnp.bfloat16) for g, f in zip(gained, factors)]
    return (*(lax.all_gather(w, "rows", axis=0, tiled=True) for w in narrow), *factors)


def opposite(me, d):
    core, east, north = lax.rem(me, 2), lax.rem(me // 2, 2), me // 4
    return (
        lax.rem(north + d // 4, 2) * 4
        + lax.rem(east + (d // 2) % 2, 2) * 2
        + lax.rem(core + d % 2, 2)
    )


def parts_of(columns):
    first = 2 * LANES
    return (
        (0, 0, first, 4),
        (0, first, columns - first, 4),
        (1, 0, columns, 8),
        (2, 0, columns, 8),
    )


def late_pairs(parts, p):
    return {len(parts) - 2: 1, len(parts) - 1: parts[p][3] // 2}.get(p, 0)


def kernel(parts, share, gain, *refs):
    args, factors, gathered, late = refs[0:6], *refs[6:9]
    (held, wide_one, wide_other, box_first, box_next, box_rest,
     load_sem, send_sem, bulk_sem, own_sem, d_sem, box_sem, late_sem) = refs[9:]
    rows = args[0].shape[0]
    every = range(len(parts))

    me = lax.axis_index("rows")
    core = lax.rem(me, 2)
    sibling, at_x, at_y, at_d = (opposite(me, d) for d in (1, 2, 4, 6))
    near = at_x + core * (at_y - at_x)
    side = at_y + core * (at_x - at_y)

    def columns_of(p):
        return pl.ds(parts[p][1], parts[p][2])

    def load(p):
        m = parts[p][0]
        for i in (2 * m, 2 * m + 1):
            pltpu.make_async_copy(
                args[i].at[:, columns_of(p)], held.at[i, :, columns_of(p)], load_sem.at[p]
            ).start()

    def loaded(p):
        ref = held.at[pl.ds(2 * parts[p][0], 2), :, columns_of(p)]
        pltpu.make_async_copy(ref, ref, load_sem.at[p]).wait()

    load(0)

    barrier = pltpu.get_barrier_semaphore()
    for d in range(1, 8):
        pl.semaphore_signal(barrier, inc=1, device_id={"rows": opposite(me, d)}, device_id_type=MESH)

    for j in range(rows // LANES):
        s = jnp.broadcast_to(share[j * LANES:(j + 1) * LANES][None], (LANES, LANES)).T
        g = jnp.broadcast_to(gain[j * LANES:(j + 1) * LANES][None], (LANES, LANES)).T
        wide_one[j * LANES:(j + 1) * LANES, :] = s * g
        wide_other[j * LANES:(j + 1) * LANES, :] = (1.0 - s) * g

    def mix(p):
        m, _, width, _ = parts[p]

        def body(i, top):
            at = pl.ds(pl.multiple_of(i * 8, 8), 8)
            a = jnp.concatenate([wide_one[at, :]] * (width // LANES), axis=1)
            b = jnp.concatenate([wide_other[at, :]] * (width // LANES), axis=1)
            mixed = a * held[2 * m, at, columns_of(p)] + b * held[2 * m + 1, at, columns_of(p)]
            held[2 * m, at, columns_of(p)] = mixed
            return jnp.maximum(top, jnp.abs(mixed))

        top = lax.fori_loop(0, rows // 8, body, jnp.zeros((8, width), jnp.float32), unroll=4)
        return jnp.max(top, axis=0, keepdims=True)

    def exchange(box, which):
        for d in range(1, 8):
            pltpu.make_async_remote_copy(
                box.at[me], box.at[me], box_sem.at[2 * which], box_sem.at[2 * which + 1],
                device_id={"rows": opposite(me, d)}, device_id_type=MESH,
            ).start()

    def exchanged(box, which):
        return pltpu.make_async_remote_copy(
            box.at[pl.ds(0, 7)], box.at[pl.ds(0, 7)], box_sem.at[2 * which], box_sem.at[2 * which + 1],
            device_id={"rows": sibling}, device_id_type=MESH,
        )

    def height(p):
        return rows // parts[p][3]

    def piece(p, owner, k, count=1):
        at = pl.multiple_of(owner * rows + k * height(p), 16)
        return gathered.at[parts[p][0], pl.ds(at, count * height(p)), columns_of(p)]

    def send(p, owner, k, stream, target, arrive):
        ref = piece(p, owner, k)
        pltpu.make_async_remote_copy(
            ref, ref, send_sem.at[stream], arrive, device_id={"rows": target}, device_id_type=MESH
        ).start()

    def arrived(ref, arrive, stream=0):
        return pltpu.make_async_remote_copy(
            ref, ref, send_sem.at[stream], arrive, device_id={"rows": sibling}, device_id_type=MESH
        )

    def narrow(p, k, inverse):
        m = parts[p][0]

        def body(i, _):
            at = pl.multiple_of(k * height(p) + i * 16, 16)
            small = (held[2 * m, pl.ds(at, 16), columns_of(p)] * inverse).astype(jnp.bfloat16)
            gathered[m, pl.ds(pl.multiple_of(me * rows + at, 16), 16), columns_of(p)] = small
            return 0

        lax.fori_loop(0, height(p) // 16, body, 0, unroll=True)

    def send_own(p, k):
        send(p, me, k, OWN_X, at_x, own_sem.at[p, k])
        send(p, me, k, OWN_Y, at_y, own_sem.at[p, k])
        send(p, me, k, OWN_S, sibling, bulk_sem.at[OWN_S])

    def narrow_and_send(p, factor, sent):
        factors[parts[p][0], :, columns_of(p)] = factor
        inverse = 1.0 / factor
        for k in range(parts[p][3]):
            narrow(p, k, inverse)
            if 1 <= k <= sent:
                send_own(p, k - 1)
        if sent == parts[p][3]:
            send_own(p, sent - 1)

    loaded(0)
    load(1)
    box_first[me] = mix(0)
    pl.semaphore_wait(barrier, 7)
    exchange(box_first, 0)
    exchanged(box_first, 0).wait_recv()
    narrow_and_send(0, jnp.max(box_first[...], axis=0), 1)
    loaded(1)
    load(2)
    load(3)
    box_next[me] = mix(1)
    exchange(box_next, 1)
    for k in range(1, parts[0][3]):
        send_own(0, k)
    exchanged(box_next, 1).wait_recv()
    narrow_and_send(1, jnp.max(box_next[...], axis=0), parts[1][3] // 2)
    loaded(2)
    box_rest[me, 0:1] = mix(2)
    loaded(3)
    box_rest[me, 1:2] = mix(3)
    exchange(box_rest, 2)
    for k in range(parts[1][3] // 2, parts[1][3]):
        send_own(1, k)
    exchanged(box_rest, 2).wait_recv()
    both = jnp.max(box_rest[...], axis=0)
    for p in (2, 3):
        narrow_and_send(p, both[p - 2:p - 1], parts[p][3])

    aside = 0
    for p in every:
        chunks = parts[p][3]
        half = chunks // 2
        for k in range(chunks):
            arrived(piece(p, 0, 0, 2), own_sem.at[p, k]).wait_recv()
            send(p, at_x, k, X_S, sibling, bulk_sem.at[X_S])
            send(p, at_y, k, Y_S, sibling, bulk_sem.at[Y_S])
            j = k % half
            if j >= late_pairs(parts, p):
                if k < half:
                    send(p, at_x, k, DIAG, at_y, d_sem.at[p, j])
                else:
                    send(p, at_y, k, DIAG, at_x, d_sem.at[p, j])
            elif k >= half:
                send(p, near, j + core * half, DIAG, side, d_sem.at[p, j])
                pltpu.make_async_copy(
                    piece(p, side, j + (1 - core) * half),
                    late.at[pl.ds(aside, height(p)), :],
                    late_sem,
                ).start()
                aside += height(p)
    for p in every:
        half = parts[p][3] // 2
        for j in range(half):
            if j >= late_pairs(parts, p):
                arrived(piece(p, 0, 0, 2), d_sem.at[p, j]).wait_recv()
                send(p, at_d, j, D_S, sibling, bulk_sem.at[D_S])
                send(p, at_d, j + half, D_S, sibling, bulk_sem.at[D_S])
            else:
                arrived(piece(p, 0, 0, 1), d_sem.at[p, j]).wait_recv()
                send(p, at_d, j + core * half, D_S, sibling, bulk_sem.at[D_S])

    matrices = gathered.at[:, pl.ds(0, rows), :]
    relayed = gathered.at[0, pl.ds(0, 3 * rows - late.shape[0]), :]
    for stream in range(7):
        moved = arrived(relayed if stream in (DIAG, D_S) else matrices, bulk_sem.at[stream], stream)
        if stream in (OWN_S, X_S, Y_S, D_S):
            moved.wait_recv()
        moved.wait_send()
    pltpu.make_async_copy(gathered.at[0, pl.ds(0, late.shape[0]), :], late, late_sem).wait()
    for which, box in enumerate((box_first, box_next, box_rest)):
        exchanged(box, which).wait_send()


def settle(parts, factors, gathered, *refs):
    targets, sems = refs[:6], refs[6]
    rows = gathered.shape[1] // 8
    me = lax.axis_index("rows")
    copies = []

    def write(m, at, size):
        at = pl.multiple_of(at, 16)
        copies.append(
            pltpu.make_async_copy(
                gathered.at[m, pl.ds(at, size), :], targets[m].at[pl.ds(at, size), :], sems.at[len(copies)]
            )
        )

    for p in range(len(parts) - 3, len(parts)):
        m, _, _, chunks = parts[p]
        height, half = rows // chunks, chunks // 2
        for d in range(8):
            owner = opposite(me, d)
            core = lax.rem(owner, 2)
            late = late_pairs(parts, p)
            if late == 0 or d < 6:
                write(m, owner * rows, rows)
            elif late == half:
                write(m, owner * rows + core * half * height, half * height)
            else:
                write(m, owner * rows + core * late * height, half * height)
                write(m, owner * rows + (half + late) * height, (half - late) * height)
    for c in copies:
        c.start()
    for m in range(3):
        targets[3 + m][...] = factors[m, 0]
    for c in copies:
        c.wait()


def finish(parts, mine, other, key, value, out_key, out_value, sems):
    rows = value.shape[0] // 8
    me = lax.axis_index("rows")
    copies = []
    for d, late in ((6, mine), (7, other)):
        owner = opposite(me, d)
        core = lax.rem(owner, 2)
        start = 0
        for p, out in ((len(parts) - 2, out_key), (len(parts) - 1, out_value)):
            chunks = parts[p][3]
            size = rows // chunks * late_pairs(parts, p)
            at = pl.multiple_of(owner * rows + (1 - core) * (rows // 2), 16)
            copies.append(
                pltpu.make_async_copy(
                    late.at[pl.ds(start, size), :], out.at[pl.ds(at, size), :], sems.at[len(copies)]
                )
            )
            start += size
    for c in copies:
        c.start()
    for c in copies:
        c.wait()


def gathered_by_kernel(*arrays):
    *weights, mix_share, norm_gain = arrays
    rows, columns = weights[0].shape
    parts = parts_of(columns)
    most = max(part[3] for part in parts)
    late_rows = sum(rows // part[3] * late_pairs(parts, p) for p, part in enumerate(parts))
    vmem, hbm = pl.BlockSpec(memory_space=pltpu.VMEM), pl.BlockSpec(memory_space=pltpu.HBM)
    anywhere = pl.BlockSpec(memory_space=pl.ANY)
    dma = pltpu.SemaphoreType.DMA
    results = pl.pallas_call(
        functools.partial(kernel, parts),
        out_shape=[
            pltpu.VMEM((3, 1, columns), jnp.float32),
            pltpu.VMEM((3, 8 * rows, columns), jnp.bfloat16),
            pltpu.VMEM((late_rows, columns), jnp.bfloat16),
        ],
        in_specs=[vmem] * 2 + [hbm] * 6,
        out_specs=[vmem] * 3,
        scratch_shapes=[
            pltpu.VMEM((6, rows, columns), jnp.float32),
            pltpu.VMEM((rows, LANES), jnp.float32),
            pltpu.VMEM((rows, LANES), jnp.float32),
            pltpu.VMEM((8, 1, parts[0][2]), jnp.float32),
            pltpu.VMEM((8, 1, parts[1][2]), jnp.float32),
            pltpu.VMEM((8, 2, columns), jnp.float32),
            dma((4,)),
            dma((7,)),
            dma((7,)),
            dma((4, most)),
            dma((4, most // 2)),
            dma((6,)),
            dma(()),
        ],
        compiler_params=pltpu.CompilerParams(
            collective_id=0, has_side_effects=True, vmem_limit_bytes=21 * 2**20
        ),
    )(mix_share, norm_gain, *weights)
    factors, gathered, late = [pltpu.with_memory_space_constraint(r, pltpu.VMEM) for r in results]
    whole = jax.ShapeDtypeStruct((8 * rows, columns), jnp.bfloat16)
    mine = lax.ppermute(late, "rows", [(i, i ^ (2, 4)[i % 2]) for i in range(8)])
    query, key, value, *factors = pl.pallas_call(
        functools.partial(settle, parts),
        out_shape=[whole] * 3 + [jax.ShapeDtypeStruct((columns,), jnp.float32)] * 3,
        in_specs=[vmem] * 2,
        out_specs=[anywhere] * 3 + [vmem] * 3,
        scratch_shapes=[dma((26,))],
        cost_estimate=pl.CostEstimate(flops=0, bytes_accessed=48 * rows * columns, transcendentals=0),
        compiler_params=pltpu.CompilerParams(vmem_limit_bytes=2**20),
    )(factors, gathered)
    mine, key, value = lax.optimization_barrier((mine, key, value))
    other = lax.ppermute(mine, "rows", [(i, i ^ 1) for i in range(8)])
    key, value = pl.pallas_call(
        functools.partial(finish, parts),
        out_shape=[whole] * 2,
        in_specs=[vmem] * 2 + [anywhere] * 2,
        out_specs=[anywhere] * 2,
        scratch_shapes=[dma((4,))],
        input_output_aliases={2: 0, 3: 1},
        compiler_params=pltpu.CompilerParams(vmem_limit_bytes=2**20),
    )(mine, other, key, value)
    return query, key, value, *factors


def solution(mesh):
    placed = (P("rows", "model"),) * 6 + (P("rows"),) * 2
    local = gathered_by_kernel if mesh.shape["rows"] == 8 else gathered_by_collectives
    return jax.shard_map(
        local,
        mesh=mesh,
        in_specs=placed,
        out_specs=(P(None, "model"),) * 3 + (P("model"),) * 3,
        check_vma=False,
    )
```

```python
import functools

import jax
import jax.numpy as jnp
from jax import lax
from jax.experimental import pallas as pl
from jax.experimental.pallas import tpu as pltpu
from jax.sharding import PartitionSpec as P

MESH = pl.DeviceIdType.MESH
LANES = 128
OWN_X, OWN_Y, OWN_S, DIAG, X_S, Y_S, D_S = range(7)


def gathered_by_collectives(one_query, other_query, one_key, other_key, one_value, other_value, mix_share, norm_gain):
    share, gain = mix_share[:, None], norm_gain[:, None]
    gained = [
        (share * one + (1.0 - share) * other) * gain
        for one, other in ((one_query, other_query), (one_key, other_key), (one_value, other_value))
    ]
    factors = lax.pmax(tuple(jnp.max(jnp.abs(g), axis=0) for g in gained), "rows")
    narrow = [(g / f).astype(jnp.bfloat16) for g, f in zip(gained, factors)]
    return (*(lax.all_gather(w, "rows", axis=0, tiled=True) for w in narrow), *factors)


def opposite(me, d):
    core, east, north = lax.rem(me, 2), lax.rem(me // 2, 2), me // 4
    return (
        lax.rem(north + d // 4, 2) * 4
        + lax.rem(east + (d // 2) % 2, 2) * 2
        + lax.rem(core + d % 2, 2)
    )


def parts_of(columns):
    first = 2 * LANES
    return (
        (0, 0, first, 10),
        (0, first, columns - first, 2),
        (1, 0, columns, 8),
        (2, 0, columns, 8),
    )


def late_pairs(parts, p):
    return {len(parts) - 2: 1, len(parts) - 1: parts[p][3] // 2}.get(p, 0)


def kernel(parts, share, gain, *refs):
    args, factors, gathered, late = refs[0:6], *refs[6:9]
    (held, wide_one, wide_other, box_first, box_next, box_rest, early,
     load_sem, send_sem, bulk_sem, own_sem, d_sem, box_sem, late_sem, early_sem) = refs[9:]
    rows, columns = args[0].shape
    every = range(len(parts))
    base = [sum(part[3] for part in parts[:p]) for p in every]

    me = lax.axis_index("rows")
    core = lax.rem(me, 2)
    sibling, at_x, at_y, at_d = (opposite(me, d) for d in (1, 2, 4, 6))
    near = at_x + core * (at_y - at_x)
    side = at_y + core * (at_x - at_y)

    def columns_of(p):
        return pl.ds(parts[p][1], parts[p][2])

    def load(p):
        m = parts[p][0]
        for i in (2 * m, 2 * m + 1):
            pltpu.make_async_copy(
                args[i].at[:, columns_of(p)], held.at[i, :, columns_of(p)], load_sem.at[p]
            ).start()

    def loaded(p):
        ref = held.at[pl.ds(2 * parts[p][0], 2), :, columns_of(p)]
        pltpu.make_async_copy(ref, ref, load_sem.at[p]).wait()

    load(0)

    barrier = pltpu.get_barrier_semaphore()
    for d in range(1, 8):
        pl.semaphore_signal(barrier, inc=1, device_id={"rows": opposite(me, d)}, device_id_type=MESH)

    for j in range(rows // LANES):
        s = jnp.broadcast_to(share[j * LANES:(j + 1) * LANES][None], (LANES, LANES)).T
        g = jnp.broadcast_to(gain[j * LANES:(j + 1) * LANES][None], (LANES, LANES)).T
        wide_one[j * LANES:(j + 1) * LANES, :] = s * g
        wide_other[j * LANES:(j + 1) * LANES, :] = (1.0 - s) * g

    def mix(p):
        m, _, width, _ = parts[p]

        def body(i, top):
            at = pl.ds(pl.multiple_of(i * 8, 8), 8)
            a = jnp.concatenate([wide_one[at, :]] * (width // LANES), axis=1)
            b = jnp.concatenate([wide_other[at, :]] * (width // LANES), axis=1)
            mixed = a * held[2 * m, at, columns_of(p)] + b * held[2 * m + 1, at, columns_of(p)]
            held[2 * m, at, columns_of(p)] = mixed
            return jnp.maximum(top, jnp.abs(mixed))

        top = lax.fori_loop(0, rows // 8, body, jnp.zeros((8, width), jnp.float32), unroll=4)
        return jnp.max(top, axis=0, keepdims=True)

    def exchange(box, which):
        for d in (6, 7, 2, 4, 3, 5, 1):
            pltpu.make_async_remote_copy(
                box.at[me], box.at[me], box_sem.at[2 * which], box_sem.at[2 * which + 1],
                device_id={"rows": opposite(me, d)}, device_id_type=MESH,
            ).start()

    def exchanged(box, which):
        return pltpu.make_async_remote_copy(
            box.at[pl.ds(0, 7)], box.at[pl.ds(0, 7)], box_sem.at[2 * which], box_sem.at[2 * which + 1],
            device_id={"rows": sibling}, device_id_type=MESH,
        )

    def height(p):
        return rows // parts[p][3]

    def piece(p, owner, k, count=1):
        at = pl.multiple_of(owner * rows + k * height(p), 16)
        return gathered.at[parts[p][0], pl.ds(at, count * height(p)), columns_of(p)]

    def send(p, owner, k, stream, target, arrive):
        ref = piece(p, owner, k)
        pltpu.make_async_remote_copy(
            ref, ref, send_sem.at[stream], arrive, device_id={"rows": target}, device_id_type=MESH
        ).start()

    def arrived(ref, arrive, stream=0):
        return pltpu.make_async_remote_copy(
            ref, ref, send_sem.at[stream], arrive, device_id={"rows": sibling}, device_id_type=MESH
        )

    def narrow(p, k, inverse):
        m = parts[p][0]

        def body(i, _):
            at = pl.multiple_of(k * height(p) + i * 16, 16)
            small = (held[2 * m, pl.ds(at, 16), columns_of(p)] * inverse).astype(jnp.bfloat16)
            gathered[m, pl.ds(pl.multiple_of(me * rows + at, 16), 16), columns_of(p)] = small
            return 0

        lax.fori_loop(0, height(p) // 16, body, 0, unroll=True)

    def send_own(p, k):
        if p or k not in ahead:
            send(p, me, k, OWN_X, at_x, own_sem.at[base[p] + k])
            send(p, me, k, OWN_Y, at_y, own_sem.at[base[p] + k])
        send(p, me, k, OWN_S, sibling, bulk_sem.at[OWN_S])

    def narrow_and_send(p, factor, sent):
        factors[parts[p][0], :, columns_of(p)] = factor
        inverse = 1.0 / factor
        for k in range(parts[p][3]):
            narrow(p, k, inverse)
            if 1 <= k <= sent:
                send_own(p, k - 1)
        if sent == parts[p][3]:
            send_own(p, sent - 1)

    ahead = (0, parts[0][3] // 2)

    def send_early():
        for place, target in enumerate((at_x, at_y)):
            for i, k in enumerate(ahead):
                pltpu.make_async_remote_copy(
                    held.at[0, pl.ds(k * height(0), height(0)), columns_of(0)],
                    early.at[place, i],
                    early_sem.at[0],
                    early_sem.at[1],
                    device_id={"rows": target},
                    device_id_type=MESH,
                ).start()

    early_all = pltpu.make_async_remote_copy(
        early, early, early_sem.at[0], early_sem.at[1], device_id={"rows": at_x}, device_id_type=MESH
    )

    def narrow_early():
        early_all.wait_recv()
        inverse = 1.0 / factors[0, :, columns_of(0)]
        for place, owner in enumerate((at_x, at_y)):
            for i, k in enumerate(ahead):
                for r in range(0, height(0), 16):
                    at = pl.multiple_of(owner * rows + k * height(0) + r, 16)
                    small = (early[place, i, r:r + 16, :] * inverse).astype(jnp.bfloat16)
                    gathered[0, pl.ds(at, 16), columns_of(0)] = small

    loaded(0)
    load(1)
    box_first[me] = mix(0)
    pl.semaphore_wait(barrier, 7)
    exchange(box_first, 0)
    send_early()
    exchanged(box_first, 0).wait_recv()
    narrow_and_send(0, jnp.max(box_first[...], axis=0), 3)
    loaded(1)
    load(2)
    load(3)
    box_next[me] = mix(1)
    exchange(box_next, 1)
    for k in range(3, parts[0][3]):
        send_own(0, k)
    narrow_early()
    exchanged(box_next, 1).wait_recv()
    narrow_and_send(1, jnp.max(box_next[...], axis=0), parts[1][3] // 2)
    loaded(2)
    box_rest[me, 0:1] = mix(2)
    loaded(3)
    box_rest[me, 1:2] = mix(3)
    exchange(box_rest, 2)
    for k in range(parts[1][3] // 2, parts[1][3]):
        send_own(1, k)
    exchanged(box_rest, 2).wait_recv()
    both = jnp.max(box_rest[...], axis=0)
    for p in (2, 3):
        narrow_and_send(p, both[p - 2:p - 1], parts[p][3])

    aside = 0
    for p in every:
        chunks = parts[p][3]
        half = chunks // 2
        for k in range(chunks):
            if p or k not in ahead:
                arrived(piece(p, 0, 0, 2), own_sem.at[base[p] + k]).wait_recv()
            send(p, at_x, k, X_S, sibling, bulk_sem.at[X_S])
            send(p, at_y, k, Y_S, sibling, bulk_sem.at[Y_S])
            j = k % half
            if j >= late_pairs(parts, p):
                if k < half:
                    send(p, at_x, k, DIAG, at_y, d_sem.at[base[p] // 2 + j])
                else:
                    send(p, at_y, k, DIAG, at_x, d_sem.at[base[p] // 2 + j])
            elif k >= half:
                send(p, near, j + core * half, DIAG, side, d_sem.at[base[p] // 2 + j])
                pltpu.make_async_copy(
                    piece(p, side, j + (1 - core) * half),
                    late.at[pl.ds(aside, height(p)), :],
                    late_sem,
                ).start()
                aside += height(p)
    for p in every:
        half = parts[p][3] // 2
        for j in range(half):
            if j >= late_pairs(parts, p):
                arrived(piece(p, 0, 0, 2), d_sem.at[base[p] // 2 + j]).wait_recv()
                send(p, at_d, j, D_S, sibling, bulk_sem.at[D_S])
                send(p, at_d, j + half, D_S, sibling, bulk_sem.at[D_S])
            else:
                arrived(piece(p, 0, 0, 1), d_sem.at[base[p] // 2 + j]).wait_recv()
                send(p, at_d, j + core * half, D_S, sibling, bulk_sem.at[D_S])

    width = parts[0][2]
    sizes = {
        stream: gathered.at[:, pl.ds(0, rows), :] for stream in (OWN_S, X_S, Y_S)
    } | {
        stream: gathered.at[0, pl.ds(0, 3 * rows - late.shape[0]), :] for stream in (DIAG, D_S)
    } | {
        stream: gathered.at[pl.ds(0, 2), pl.ds(0, 3 * rows * columns // (2 * width) - height(0)), pl.ds(0, width)]
        for stream in (OWN_X, OWN_Y)
    }
    for stream, size in sizes.items():
        moved = arrived(size, bulk_sem.at[stream], stream)
        if stream in (OWN_S, X_S, Y_S, D_S):
            moved.wait_recv()
        moved.wait_send()
    early_all.wait_send()
    pltpu.make_async_copy(gathered.at[0, pl.ds(0, late.shape[0]), :], late, late_sem).wait()
    for which, box in enumerate((box_first, box_next, box_rest)):
        exchanged(box, which).wait_send()


def settle(parts, factors, gathered, *refs):
    targets, sems = refs[:6], refs[6]
    rows = gathered.shape[1] // 8
    me = lax.axis_index("rows")
    copies = []

    def write(m, at, size):
        at = pl.multiple_of(at, 16)
        copies.append(
            pltpu.make_async_copy(
                gathered.at[m, pl.ds(at, size), :], targets[m].at[pl.ds(at, size), :], sems.at[len(copies)]
            )
        )

    for p in range(len(parts) - 3, len(parts)):
        m, _, _, chunks = parts[p]
        height, half = rows // chunks, chunks // 2
        for d in range(8):
            owner = opposite(me, d)
            core = lax.rem(owner, 2)
            late = late_pairs(parts, p)
            if late == 0 or d < 6:
                write(m, owner * rows, rows)
            elif late == half:
                write(m, owner * rows + core * half * height, half * height)
            else:
                write(m, owner * rows + core * late * height, half * height)
                write(m, owner * rows + (half + late) * height, (half - late) * height)
    for c in copies:
        c.start()
    for m in range(3):
        targets[3 + m][...] = factors[m, 0]
    for c in copies:
        c.wait()


def finish(parts, d, late, key, value, out_key, out_value, sems):
    rows = value.shape[0] // 8
    owner = opposite(lax.axis_index("rows"), d)
    at = pl.multiple_of(owner * rows + (1 - lax.rem(owner, 2)) * (rows // 2), 16)
    copies, start = [], 0
    for p, out in ((len(parts) - 2, out_key), (len(parts) - 1, out_value)):
        size = rows // parts[p][3] * late_pairs(parts, p)
        copies.append(
            pltpu.make_async_copy(
                late.at[pl.ds(start, size), :], out.at[pl.ds(at, size), :], sems.at[len(copies)]
            )
        )
        start += size
    for c in copies:
        c.start()
    for c in copies:
        c.wait()


def gathered_by_kernel(*arrays):
    *weights, mix_share, norm_gain = arrays
    rows, columns = weights[0].shape
    parts = parts_of(columns)
    late_rows = sum(rows // part[3] * late_pairs(parts, p) for p, part in enumerate(parts))
    vmem, hbm = pl.BlockSpec(memory_space=pltpu.VMEM), pl.BlockSpec(memory_space=pltpu.HBM)
    anywhere = pl.BlockSpec(memory_space=pl.ANY)
    dma = pltpu.SemaphoreType.DMA
    results = pl.pallas_call(
        functools.partial(kernel, parts),
        out_shape=[
            pltpu.VMEM((3, 1, columns), jnp.float32),
            pltpu.VMEM((3, 8 * rows, columns), jnp.bfloat16),
            pltpu.VMEM((late_rows, columns), jnp.bfloat16),
        ],
        in_specs=[vmem] * 2 + [hbm] * 6,
        out_specs=[vmem] * 3,
        scratch_shapes=[
            pltpu.VMEM((6, rows, columns), jnp.float32),
            pltpu.VMEM((rows, LANES), jnp.float32),
            pltpu.VMEM((rows, LANES), jnp.float32),
            pltpu.VMEM((8, 1, parts[0][2]), jnp.float32),
            pltpu.VMEM((8, 1, parts[1][2]), jnp.float32),
            pltpu.VMEM((8, 2, columns), jnp.float32),
            pltpu.VMEM((2, 2, rows // parts[0][3], parts[0][2]), jnp.float32),
            dma((4,)),
            dma((7,)),
            dma((7,)),
            dma((sum(part[3] for part in parts),)),
            dma((sum(part[3] // 2 for part in parts),)),
            dma((6,)),
            dma(()),
            dma((2,)),
        ],
        compiler_params=pltpu.CompilerParams(
            collective_id=0, has_side_effects=True, vmem_limit_bytes=21 * 2**20
        ),
    )(mix_share, norm_gain, *weights)
    factors, gathered, late = [pltpu.with_memory_space_constraint(r, pltpu.VMEM) for r in results]
    whole = jax.ShapeDtypeStruct((8 * rows, columns), jnp.bfloat16)
    mine = lax.ppermute(late, "rows", [(i, i ^ (2, 4)[i % 2]) for i in range(8)])
    query, key, value, *factors = pl.pallas_call(
        functools.partial(settle, parts),
        out_shape=[whole] * 3 + [jax.ShapeDtypeStruct((columns,), jnp.float32)] * 3,
        in_specs=[vmem] * 2,
        out_specs=[anywhere] * 3 + [vmem] * 3,
        scratch_shapes=[dma((26,))],
        cost_estimate=pl.CostEstimate(flops=0, bytes_accessed=48 * rows * columns, transcendentals=0),
        compiler_params=pltpu.CompilerParams(vmem_limit_bytes=2**20),
    )(factors, gathered)
    mine, key, value = lax.optimization_barrier((mine, key, value))
    other = lax.ppermute(mine, "rows", [(i, i ^ 1) for i in range(8)])
    for d, late in ((6, mine), (7, other)):
        key, value = pl.pallas_call(
            functools.partial(finish, parts, d),
            out_shape=[whole] * 2,
            in_specs=[vmem] + [anywhere] * 2,
            out_specs=[anywhere] * 2,
            scratch_shapes=[dma((2,))],
            input_output_aliases={1: 0, 2: 1},
            cost_estimate=pl.CostEstimate(flops=0, bytes_accessed=4 * late_rows * columns, transcendentals=0),
            compiler_params=pltpu.CompilerParams(vmem_limit_bytes=2**20),
        )(late, key, value)
    return query, key, value, *factors


def solution(mesh):
    placed = (P("rows", "model"),) * 6 + (P("rows"),) * 2
    local = gathered_by_kernel if mesh.shape["rows"] == 8 else gathered_by_collectives
    return jax.shard_map(
        local,
        mesh=mesh,
        in_specs=placed,
        out_specs=(P(None, "model"),) * 3 + (P("model"),) * 3,
        check_vma=False,
    )
```

```python
import functools

import jax
import jax.numpy as jnp
from jax import lax
from jax.experimental import pallas as pl
from jax.experimental.pallas import tpu as pltpu
from jax.sharding import PartitionSpec as P

MESH = pl.DeviceIdType.MESH
LANES = 128
OWN_X, OWN_Y, OWN_S, DIAG, X_S, Y_S, D_S = range(7)


def gathered_by_collectives(one_query, other_query, one_key, other_key, one_value, other_value, mix_share, norm_gain):
    share, gain = mix_share[:, None], norm_gain[:, None]
    gained = [
        (share * one + (1.0 - share) * other) * gain
        for one, other in ((one_query, other_query), (one_key, other_key), (one_value, other_value))
    ]
    factors = lax.pmax(tuple(jnp.max(jnp.abs(g), axis=0) for g in gained), "rows")
    narrow = [(g / f).astype(jnp.bfloat16) for g, f in zip(gained, factors)]
    return (*(lax.all_gather(w, "rows", axis=0, tiled=True) for w in narrow), *factors)


def opposite(me, d):
    core, east, north = lax.rem(me, 2), lax.rem(me // 2, 2), me // 4
    return (
        lax.rem(north + d // 4, 2) * 4
        + lax.rem(east + (d // 2) % 2, 2) * 2
        + lax.rem(core + d % 2, 2)
    )


def parts_of(columns):
    first = 2 * LANES
    return (
        (0, 0, first, 10),
        (0, first, columns - first, 2),
        (1, 0, columns, 8),
        (2, 0, columns, 8),
    )


def late_pairs(parts, p):
    return {len(parts) - 2: 1, len(parts) - 1: parts[p][3] // 2}.get(p, 0)


def kernel(parts, *refs):
    args, factors, gathered, late, closing = refs[0:8], *refs[8:12]
    (held, share, gain, wide_one, wide_other, box_first, box_next, box_rest, early,
     load_sem, send_sem, bulk_sem, own_sem, d_sem, box_sem, late_sem, early_sem, row_sem) = refs[12:]
    rows, columns = args[0].shape
    every = range(len(parts))
    base = [sum(part[3] for part in parts[:p]) for p in every]

    me = lax.axis_index("rows")
    core = lax.rem(me, 2)
    sibling, at_x, at_y, at_d = (opposite(me, d) for d in (1, 2, 4, 6))
    near = at_x + core * (at_y - at_x)
    side = at_y + core * (at_x - at_y)

    def columns_of(p):
        return pl.ds(parts[p][1], parts[p][2])

    def load(p):
        m = parts[p][0]
        for i in (2 * m, 2 * m + 1):
            pltpu.make_async_copy(
                args[i].at[:, columns_of(p)], held.at[i, :, columns_of(p)], load_sem.at[p]
            ).start()

    def loaded(p):
        ref = held.at[pl.ds(2 * parts[p][0], 2), :, columns_of(p)]
        pltpu.make_async_copy(ref, ref, load_sem.at[p]).wait()

    by_row = [pltpu.make_async_copy(args[6 + i], to, row_sem.at[i]) for i, to in enumerate((share, gain))]
    for c in by_row:
        c.start()
    load(0)

    barrier = pltpu.get_barrier_semaphore()
    for d in range(1, 8):
        pl.semaphore_signal(barrier, inc=1, device_id={"rows": opposite(me, d)}, device_id_type=MESH)

    for c in by_row:
        c.wait()
    for j in range(rows // LANES):
        s = jnp.broadcast_to(share[j * LANES:(j + 1) * LANES][None], (LANES, LANES)).T
        g = jnp.broadcast_to(gain[j * LANES:(j + 1) * LANES][None], (LANES, LANES)).T
        wide_one[j * LANES:(j + 1) * LANES, :] = s * g
        wide_other[j * LANES:(j + 1) * LANES, :] = (1.0 - s) * g

    def mix(p):
        m, _, width, _ = parts[p]

        def body(i, top):
            at = pl.ds(pl.multiple_of(i * 8, 8), 8)
            a = jnp.concatenate([wide_one[at, :]] * (width // LANES), axis=1)
            b = jnp.concatenate([wide_other[at, :]] * (width // LANES), axis=1)
            mixed = a * held[2 * m, at, columns_of(p)] + b * held[2 * m + 1, at, columns_of(p)]
            held[2 * m, at, columns_of(p)] = mixed
            return jnp.maximum(top, jnp.abs(mixed))

        top = lax.fori_loop(0, rows // 8, body, jnp.zeros((8, width), jnp.float32), unroll=4)
        return jnp.max(top, axis=0, keepdims=True)

    def exchange(box, which):
        for d in (6, 7, 2, 4, 3, 5, 1):
            pltpu.make_async_remote_copy(
                box.at[me], box.at[me], box_sem.at[2 * which], box_sem.at[2 * which + 1],
                device_id={"rows": opposite(me, d)}, device_id_type=MESH,
            ).start()

    def exchanged(box, which):
        return pltpu.make_async_remote_copy(
            box.at[pl.ds(0, 7)], box.at[pl.ds(0, 7)], box_sem.at[2 * which], box_sem.at[2 * which + 1],
            device_id={"rows": sibling}, device_id_type=MESH,
        )

    def height(p):
        return rows // parts[p][3]

    def piece(p, owner, k, count=1):
        at = pl.multiple_of(owner * rows + k * height(p), 16)
        return gathered.at[parts[p][0], pl.ds(at, count * height(p)), columns_of(p)]

    def send(p, owner, k, stream, target, arrive, to=None):
        ref = piece(p, owner, k)
        pltpu.make_async_remote_copy(
            ref, ref if to is None else to, send_sem.at[stream], arrive,
            device_id={"rows": target}, device_id_type=MESH,
        ).start()

    def arrived(ref, arrive, stream=0):
        return pltpu.make_async_remote_copy(
            ref, ref, send_sem.at[stream], arrive, device_id={"rows": sibling}, device_id_type=MESH
        )

    def narrow(p, k, inverse):
        m = parts[p][0]

        def body(i, _):
            at = pl.multiple_of(k * height(p) + i * 16, 16)
            small = (held[2 * m, pl.ds(at, 16), columns_of(p)] * inverse).astype(jnp.bfloat16)
            gathered[m, pl.ds(pl.multiple_of(me * rows + at, 16), 16), columns_of(p)] = small
            return 0

        lax.fori_loop(0, height(p) // 16, body, 0, unroll=True)

    def send_own(p, k):
        if p or k not in ahead:
            send(p, me, k, OWN_X, at_x, own_sem.at[base[p] + k])
            send(p, me, k, OWN_Y, at_y, own_sem.at[base[p] + k])
        send(p, me, k, OWN_S, sibling, bulk_sem.at[OWN_S])

    def narrow_and_send(p, factor, sent):
        factors[parts[p][0], :, columns_of(p)] = factor
        inverse = 1.0 / factor
        for k in range(parts[p][3]):
            narrow(p, k, inverse)
            if 1 <= k <= sent:
                send_own(p, k - 1)
        if sent == parts[p][3]:
            send_own(p, sent - 1)

    ahead = (0, parts[0][3] // 2)

    def send_early():
        for place, target in enumerate((at_x, at_y)):
            for i, k in enumerate(ahead):
                pltpu.make_async_remote_copy(
                    held.at[0, pl.ds(k * height(0), height(0)), columns_of(0)],
                    early.at[place, i],
                    early_sem.at[0],
                    early_sem.at[1],
                    device_id={"rows": target},
                    device_id_type=MESH,
                ).start()

    early_all = pltpu.make_async_remote_copy(
        early, early, early_sem.at[0], early_sem.at[1], device_id={"rows": at_x}, device_id_type=MESH
    )

    def narrow_early():
        early_all.wait_recv()
        inverse = 1.0 / factors[0, :, columns_of(0)]
        for place, owner in enumerate((at_x, at_y)):
            for i, k in enumerate(ahead):
                for r in range(0, height(0), 16):
                    at = pl.multiple_of(owner * rows + k * height(0) + r, 16)
                    small = (early[place, i, r:r + 16, :] * inverse).astype(jnp.bfloat16)
                    gathered[0, pl.ds(at, 16), columns_of(0)] = small

    loaded(0)
    load(1)
    box_first[me] = mix(0)
    pl.semaphore_wait(barrier, 7)
    exchange(box_first, 0)
    send_early()
    exchanged(box_first, 0).wait_recv()
    narrow_and_send(0, jnp.max(box_first[...], axis=0), 3)
    loaded(1)
    load(2)
    load(3)
    box_next[me] = mix(1)
    exchange(box_next, 1)
    for k in range(3, parts[0][3]):
        send_own(0, k)
    narrow_early()
    exchanged(box_next, 1).wait_recv()
    narrow_and_send(1, jnp.max(box_next[...], axis=0), parts[1][3] // 2)
    loaded(2)
    box_rest[me, 0:1] = mix(2)
    loaded(3)
    box_rest[me, 1:2] = mix(3)
    exchange(box_rest, 2)
    for k in range(parts[1][3] // 2, parts[1][3]):
        send_own(1, k)
    exchanged(box_rest, 2).wait_recv()
    both = jnp.max(box_rest[...], axis=0)
    for p in (2, 3):
        narrow_and_send(p, both[p - 2:p - 1], parts[p][3])

    def closes(p, j):
        return p == every[-1] and j == parts[p][3] // 2 - 1

    aside = 0
    for p in every:
        chunks = parts[p][3]
        half = chunks // 2
        for k in range(chunks):
            if p or k not in ahead:
                arrived(piece(p, 0, 0, 2), own_sem.at[base[p] + k]).wait_recv()
            send(p, at_x, k, X_S, sibling, bulk_sem.at[X_S])
            send(p, at_y, k, Y_S, sibling, bulk_sem.at[Y_S])
            j = k % half
            if j >= late_pairs(parts, p):
                if k < half:
                    send(p, at_x, k, DIAG, at_y, d_sem.at[base[p] // 2 + j])
                else:
                    send(p, at_y, k, DIAG, at_x, d_sem.at[base[p] // 2 + j])
            elif k >= half:
                send(
                    p, near, j + core * half, DIAG, side, d_sem.at[base[p] // 2 + j],
                    closing if closes(p, j) else None,
                )
                pltpu.make_async_copy(
                    piece(p, side, j + (1 - core) * half),
                    late.at[pl.ds(aside, height(p)), :],
                    late_sem,
                ).start()
                aside += height(p)
    for p in every:
        half = parts[p][3] // 2
        for j in range(half):
            if j >= late_pairs(parts, p):
                arrived(piece(p, 0, 0, 2), d_sem.at[base[p] // 2 + j]).wait_recv()
                send(p, at_d, j, D_S, sibling, bulk_sem.at[D_S])
                send(p, at_d, j + half, D_S, sibling, bulk_sem.at[D_S])
            else:
                arrived(piece(p, 0, 0, 1), d_sem.at[base[p] // 2 + j]).wait_recv()
                if not closes(p, j):
                    send(p, at_d, j + core * half, D_S, sibling, bulk_sem.at[D_S])

    width = parts[0][2]
    sizes = {
        stream: gathered.at[:, pl.ds(0, rows), :] for stream in (OWN_S, X_S, Y_S)
    } | {
        DIAG: gathered.at[0, pl.ds(0, 3 * rows - late.shape[0]), :],
        D_S: gathered.at[0, pl.ds(0, 3 * rows - late.shape[0] - closing.shape[0]), :],
    } | {
        stream: gathered.at[pl.ds(0, 2), pl.ds(0, 3 * rows * columns // (2 * width) - height(0)), pl.ds(0, width)]
        for stream in (OWN_X, OWN_Y)
    }
    for stream, size in sizes.items():
        moved = arrived(size, bulk_sem.at[stream], stream)
        if stream in (OWN_S, X_S, Y_S, D_S):
            moved.wait_recv()
        moved.wait_send()
    early_all.wait_send()
    pltpu.make_async_copy(gathered.at[0, pl.ds(0, late.shape[0]), :], late, late_sem).wait()
    for which, box in enumerate((box_first, box_next, box_rest)):
        exchanged(box, which).wait_send()


def settle(parts, factors, gathered, *refs):
    targets, sems = refs[:6], refs[6]
    rows = gathered.shape[1] // 8
    me = lax.axis_index("rows")
    copies = []

    def write(m, at, size):
        at = pl.multiple_of(at, 16)
        copies.append(
            pltpu.make_async_copy(
                gathered.at[m, pl.ds(at, size), :], targets[m].at[pl.ds(at, size), :], sems.at[len(copies)]
            )
        )

    for p in range(len(parts) - 3, len(parts)):
        m, _, _, chunks = parts[p]
        height, half = rows // chunks, chunks // 2
        for d in range(8):
            owner = opposite(me, d)
            core = lax.rem(owner, 2)
            late = late_pairs(parts, p)
            if late == 0 or d < 6:
                write(m, owner * rows, rows)
            elif late == half:
                write(m, owner * rows + core * half * height, (half - 1) * height)
            else:
                write(m, owner * rows + core * late * height, half * height)
                write(m, owner * rows + (half + late) * height, (half - late) * height)
    for c in copies:
        c.start()
    for m in range(3):
        targets[3 + m][...] = factors[m, 0]
    for c in copies:
        c.wait()


def finish(parts, places, *refs):
    given = refs[:len(places)]
    key, value, sems = refs[-3:]
    rows = value.shape[0] // 8
    copies = []

    def write(ref, start, size, out, at):
        at = pl.multiple_of(at, 16)
        copies.append(
            pltpu.make_async_copy(
                ref.at[pl.ds(start, size), :], out.at[pl.ds(at, size), :], sems.at[len(copies)]
            )
        )

    for ref, (closing, d) in zip(given, places):
        owner = opposite(lax.axis_index("rows"), d)
        core = lax.rem(owner, 2)
        if closing:
            write(ref, 0, ref.shape[0], value, owner * rows + (1 + core) * (rows // 2) - ref.shape[0])
            continue
        start = 0
        for p, out in ((len(parts) - 2, key), (len(parts) - 1, value)):
            size = rows // parts[p][3] * late_pairs(parts, p)
            write(ref, start, size, out, owner * rows + (1 - core) * (rows // 2))
            start += size
    for c in copies:
        c.start()
    for c in copies:
        c.wait()


def gathered_by_kernel(*arrays):
    rows, columns = arrays[0].shape
    parts = parts_of(columns)
    late_rows = sum(rows // part[3] * late_pairs(parts, p) for p, part in enumerate(parts))
    vmem, hbm = pl.BlockSpec(memory_space=pltpu.VMEM), pl.BlockSpec(memory_space=pltpu.HBM)
    anywhere = pl.BlockSpec(memory_space=pl.ANY)
    dma = pltpu.SemaphoreType.DMA
    results = pl.pallas_call(
        functools.partial(kernel, parts),
        out_shape=[
            pltpu.VMEM((3, 1, columns), jnp.float32),
            pltpu.VMEM((3, 8 * rows, columns), jnp.bfloat16),
            pltpu.VMEM((late_rows, columns), jnp.bfloat16),
            pltpu.VMEM((rows // parts[-1][3], columns), jnp.bfloat16),
        ],
        in_specs=[hbm] * 8,
        out_specs=[vmem] * 4,
        scratch_shapes=[
            pltpu.VMEM((6, rows, columns), jnp.float32),
            pltpu.VMEM((rows,), jnp.float32),
            pltpu.VMEM((rows,), jnp.float32),
            pltpu.VMEM((rows, LANES), jnp.float32),
            pltpu.VMEM((rows, LANES), jnp.float32),
            pltpu.VMEM((8, 1, parts[0][2]), jnp.float32),
            pltpu.VMEM((8, 1, parts[1][2]), jnp.float32),
            pltpu.VMEM((8, 2, columns), jnp.float32),
            pltpu.VMEM((2, 2, rows // parts[0][3], parts[0][2]), jnp.float32),
            dma((4,)),
            dma((7,)),
            dma((7,)),
            dma((sum(part[3] for part in parts),)),
            dma((sum(part[3] // 2 for part in parts),)),
            dma((6,)),
            dma(()),
            dma((2,)),
            dma((2,)),
        ],
        compiler_params=pltpu.CompilerParams(
            collective_id=0, has_side_effects=True, vmem_limit_bytes=21 * 2**20
        ),
    )(*arrays)
    factors, gathered, late, closing = [
        pltpu.with_memory_space_constraint(r, pltpu.VMEM) for r in results
    ]
    whole = jax.ShapeDtypeStruct((8 * rows, columns), jnp.bfloat16)
    siblings = [(i, i ^ 1) for i in range(8)]
    mine = lax.ppermute(late, "rows", [(i, i ^ (2, 4)[i % 2]) for i in range(8)])
    closing_other = lax.ppermute(closing, "rows", siblings)
    query, key, value, *factors = pl.pallas_call(
        functools.partial(settle, parts),
        out_shape=[whole] * 3 + [jax.ShapeDtypeStruct((columns,), jnp.float32)] * 3,
        in_specs=[vmem] * 2,
        out_specs=[anywhere] * 3 + [vmem] * 3,
        scratch_shapes=[dma((26,))],
        cost_estimate=pl.CostEstimate(flops=0, bytes_accessed=48 * rows * columns, transcendentals=0),
        compiler_params=pltpu.CompilerParams(vmem_limit_bytes=2**20),
    )(factors, gathered)
    mine, closing_other, key, value = lax.optimization_barrier((mine, closing_other, key, value))
    other = lax.ppermute(mine, "rows", siblings)
    for places, given in (
        (((False, 6), (True, 6), (True, 7)), (mine, closing, closing_other)),
        (((False, 7),), (other,)),
    ):
        n = len(given)
        key, value = pl.pallas_call(
            functools.partial(finish, parts, places),
            out_shape=[whole] * 2,
            in_specs=[vmem] * n + [anywhere] * 2,
            out_specs=[anywhere] * 2,
            scratch_shapes=[dma((n + 1,))],
            input_output_aliases={n: 0, n + 1: 1},
            cost_estimate=pl.CostEstimate(flops=0, bytes_accessed=4 * late_rows * columns, transcendentals=0),
            compiler_params=pltpu.CompilerParams(vmem_limit_bytes=2**20),
        )(*given, key, value)
    return query, key, value, *factors


def solution(mesh):
    placed = (P("rows", "model"),) * 6 + (P("rows"),) * 2
    local = gathered_by_kernel if mesh.shape["rows"] == 8 else gathered_by_collectives
    return jax.shard_map(
        local,
        mesh=mesh,
        in_specs=placed,
        out_specs=(P(None, "model"),) * 3 + (P("model"),) * 3,
        check_vma=False,
    )
```

```python
import functools

import jax
import jax.numpy as jnp
from jax import lax
from jax.experimental import pallas as pl
from jax.experimental.pallas import tpu as pltpu
from jax.sharding import PartitionSpec as P


MESH = pl.DeviceIdType.MESH
LANES = 128
OWN_X, OWN_Y, OWN_S, DIAG, X_S, Y_S, D_S = range(7)


def gathered_by_collectives(one_query, other_query, one_key, other_key, one_value, other_value, mix_share, norm_gain):
    share, gain = mix_share[:, None], norm_gain[:, None]
    gained = [
        (share * one + (1.0 - share) * other) * gain
        for one, other in ((one_query, other_query), (one_key, other_key), (one_value, other_value))
    ]
    factors = lax.pmax(tuple(jnp.max(jnp.abs(g), axis=0) for g in gained), "rows")
    narrow = [(g / f).astype(jnp.bfloat16) for g, f in zip(gained, factors)]
    return (*(lax.all_gather(w, "rows", axis=0, tiled=True) for w in narrow), *factors)


def opposite(me, d):
    core, east, north = lax.rem(me, 2), lax.rem(me // 2, 2), me // 4
    return (
        lax.rem(north + d // 4, 2) * 4
        + lax.rem(east + (d // 2) % 2, 2) * 2
        + lax.rem(core + d % 2, 2)
    )


def parts_of(columns):
    first = 2 * LANES
    return (
        (0, 0, first, 10),
        (0, first, columns - first, 2),
        (1, 0, columns, 10),
        (2, 0, columns, 10),
    )


def late_pairs(parts, p):
    return {len(parts) - 2: 3, len(parts) - 1: parts[p][3] // 2}.get(p, 0)


def kernel(parts, *refs):
    args, factors, gathered, late_key, late_value, closing = refs[0:8], *refs[8:13]
    (held, share, gain, wide_one, wide_other, box_first, box_next, box_rest, early,
     load_sem, send_sem, bulk_sem, own_sem, d_sem, box_sem, late_sem, early_sem, row_sem) = refs[13:]
    rows, columns = args[0].shape
    every = range(len(parts))
    late_rows = late_key.shape[0] + late_value.shape[0]
    base = [sum(part[3] for part in parts[:p]) for p in every]

    me = lax.axis_index("rows")
    core = lax.rem(me, 2)
    sibling, at_x, at_y, at_d = (opposite(me, d) for d in (1, 2, 4, 6))
    near = at_x + core * (at_y - at_x)
    side = at_y + core * (at_x - at_y)

    def columns_of(p):
        return pl.ds(parts[p][1], parts[p][2])

    def load(p):
        m = parts[p][0]
        for i in (2 * m, 2 * m + 1):
            pltpu.make_async_copy(
                args[i].at[:, columns_of(p)], held.at[i, :, columns_of(p)], load_sem.at[p]
            ).start()

    def loaded(p):
        ref = held.at[pl.ds(2 * parts[p][0], 2), :, columns_of(p)]
        pltpu.make_async_copy(ref, ref, load_sem.at[p]).wait()

    by_row = [pltpu.make_async_copy(args[6 + i], to, row_sem.at[i]) for i, to in enumerate((share, gain))]
    for c in by_row:
        c.start()
    load(0)

    barrier = pltpu.get_barrier_semaphore()
    for d in range(1, 8):
        pl.semaphore_signal(barrier, inc=1, device_id={"rows": opposite(me, d)}, device_id_type=MESH)

    for c in by_row:
        c.wait()
    for j in range(rows // LANES):
        s = jnp.broadcast_to(share[j * LANES:(j + 1) * LANES][None], (LANES, LANES)).T
        g = jnp.broadcast_to(gain[j * LANES:(j + 1) * LANES][None], (LANES, LANES)).T
        wide_one[j * LANES:(j + 1) * LANES, :] = s * g
        wide_other[j * LANES:(j + 1) * LANES, :] = (1.0 - s) * g

    def mix(p):
        m, _, width, _ = parts[p]

        def body(i, top):
            at = pl.ds(pl.multiple_of(i * 8, 8), 8)
            a = jnp.concatenate([wide_one[at, :]] * (width // LANES), axis=1)
            b = jnp.concatenate([wide_other[at, :]] * (width // LANES), axis=1)
            mixed = a * held[2 * m, at, columns_of(p)] + b * held[2 * m + 1, at, columns_of(p)]
            held[2 * m, at, columns_of(p)] = mixed
            return jnp.maximum(top, jnp.abs(mixed))

        top = lax.fori_loop(0, rows // 8, body, jnp.zeros((8, width), jnp.float32), unroll=4)
        return jnp.max(top, axis=0, keepdims=True)

    def exchange(box, which):
        for d in (6, 7, 2, 4, 3, 5, 1):
            pltpu.make_async_remote_copy(
                box.at[me], box.at[me], box_sem.at[2 * which], box_sem.at[2 * which + 1],
                device_id={"rows": opposite(me, d)}, device_id_type=MESH,
            ).start()

    def exchanged(box, which):
        return pltpu.make_async_remote_copy(
            box.at[pl.ds(0, 7)], box.at[pl.ds(0, 7)], box_sem.at[2 * which], box_sem.at[2 * which + 1],
            device_id={"rows": sibling}, device_id_type=MESH,
        )

    def height(p):
        return rows // parts[p][3]

    def piece(p, owner, k, count=1):
        at = pl.multiple_of(owner * rows + k * height(p), 16)
        return gathered.at[parts[p][0], pl.ds(at, count * height(p)), columns_of(p)]

    def send(p, owner, k, stream, target, arrive, to=None):
        ref = piece(p, owner, k)
        pltpu.make_async_remote_copy(
            ref, ref if to is None else to, send_sem.at[stream], arrive,
            device_id={"rows": target}, device_id_type=MESH,
        ).start()

    def arrived(ref, arrive, stream=0):
        return pltpu.make_async_remote_copy(
            ref, ref, send_sem.at[stream], arrive, device_id={"rows": sibling}, device_id_type=MESH
        )

    def narrow(p, k, inverse):
        m = parts[p][0]

        def body(i, _):
            at = pl.multiple_of(k * height(p) + i * 16, 16)
            small = (held[2 * m, pl.ds(at, 16), columns_of(p)] * inverse).astype(jnp.bfloat16)
            gathered[m, pl.ds(pl.multiple_of(me * rows + at, 16), 16), columns_of(p)] = small
            return 0

        lax.fori_loop(0, height(p) // 16, body, 0, unroll=True)

    def send_own(p, k):
        if p or k not in ahead:
            send(p, me, k, OWN_X, at_x, own_sem.at[base[p] + k])
            send(p, me, k, OWN_Y, at_y, own_sem.at[base[p] + k])
        send(p, me, k, OWN_S, sibling, bulk_sem.at[OWN_S])

    def narrow_and_send(p, factor, sent):
        factors[parts[p][0], :, columns_of(p)] = factor
        inverse = 1.0 / factor
        for k in range(parts[p][3]):
            narrow(p, k, inverse)
            if 1 <= k <= sent:
                send_own(p, k - 1)
        if sent == parts[p][3]:
            send_own(p, sent - 1)

    ahead = (0, parts[0][3] // 2)

    def send_early():
        for place, target in enumerate((at_x, at_y)):
            for i, k in enumerate(ahead):
                pltpu.make_async_remote_copy(
                    held.at[0, pl.ds(k * height(0), height(0)), columns_of(0)],
                    early.at[place, i],
                    early_sem.at[0],
                    early_sem.at[1],
                    device_id={"rows": target},
                    device_id_type=MESH,
                ).start()

    early_all = pltpu.make_async_remote_copy(
        early, early, early_sem.at[0], early_sem.at[1], device_id={"rows": at_x}, device_id_type=MESH
    )

    def narrow_early():
        early_all.wait_recv()
        inverse = 1.0 / factors[0, :, columns_of(0)]
        for place, owner in enumerate((at_x, at_y)):
            for i, k in enumerate(ahead):
                for r in range(0, height(0), 16):
                    at = pl.multiple_of(owner * rows + k * height(0) + r, 16)
                    small = (early[place, i, r:r + 16, :] * inverse).astype(jnp.bfloat16)
                    gathered[0, pl.ds(at, 16), columns_of(0)] = small

    loaded(0)
    load(1)
    box_first[me] = mix(0)
    pl.semaphore_wait(barrier, 7)
    exchange(box_first, 0)
    send_early()
    exchanged(box_first, 0).wait_recv()
    narrow_and_send(0, jnp.max(box_first[...], axis=0), 3)
    loaded(1)
    load(2)
    load(3)
    box_next[me] = mix(1)
    exchange(box_next, 1)
    for k in range(3, parts[0][3]):
        send_own(0, k)
    narrow_early()
    exchanged(box_next, 1).wait_recv()
    narrow_and_send(1, jnp.max(box_next[...], axis=0), parts[1][3] // 2)
    loaded(2)
    box_rest[me, 0:1] = mix(2)
    loaded(3)
    box_rest[me, 1:2] = mix(3)
    exchange(box_rest, 2)
    for k in range(parts[1][3] // 2, parts[1][3]):
        send_own(1, k)
    exchanged(box_rest, 2).wait_recv()
    both = jnp.max(box_rest[...], axis=0)
    for p in (2, 3):
        narrow_and_send(p, both[p - 2:p - 1], parts[p][3])

    def closes(p, j):
        return p == every[-1] and j == parts[p][3] // 2 - 1

    for p in every:
        chunks = parts[p][3]
        half = chunks // 2
        for k in range(chunks):
            if p or k not in ahead:
                arrived(piece(p, 0, 0, 2), own_sem.at[base[p] + k]).wait_recv()
            send(p, at_x, k, X_S, sibling, bulk_sem.at[X_S])
            send(p, at_y, k, Y_S, sibling, bulk_sem.at[Y_S])
            j = k % half
            if j >= late_pairs(parts, p):
                if k < half:
                    send(p, at_x, k, DIAG, at_y, d_sem.at[base[p] // 2 + j])
                else:
                    send(p, at_y, k, DIAG, at_x, d_sem.at[base[p] // 2 + j])
            elif k >= half:
                send(
                    p, near, j + core * half, DIAG, side, d_sem.at[base[p] // 2 + j],
                    closing if closes(p, j) else None,
                )
                pltpu.make_async_copy(
                    piece(p, side, j + (1 - core) * half),
                    (late_value if p == every[-1] else late_key).at[pl.ds(j * height(p), height(p)), :],
                    late_sem,
                ).start()
    for p in every:
        half = parts[p][3] // 2
        for j in range(half):
            if j >= late_pairs(parts, p):
                arrived(piece(p, 0, 0, 2), d_sem.at[base[p] // 2 + j]).wait_recv()
                send(p, at_d, j, D_S, sibling, bulk_sem.at[D_S])
                send(p, at_d, j + half, D_S, sibling, bulk_sem.at[D_S])
            else:
                arrived(piece(p, 0, 0, 1), d_sem.at[base[p] // 2 + j]).wait_recv()
                if not closes(p, j):
                    send(p, at_d, j + core * half, D_S, sibling, bulk_sem.at[D_S])

    width = parts[0][2]
    sizes = {
        stream: gathered.at[:, pl.ds(0, rows), :] for stream in (OWN_S, X_S, Y_S)
    } | {
        DIAG: gathered.at[0, pl.ds(0, 3 * rows - late_rows), :],
        D_S: gathered.at[0, pl.ds(0, 3 * rows - late_rows - closing.shape[0]), :],
    } | {
        stream: gathered.at[pl.ds(0, 2), pl.ds(0, 3 * rows * columns // (2 * width) - height(0)), pl.ds(0, width)]
        for stream in (OWN_X, OWN_Y)
    }
    for stream, size in sizes.items():
        moved = arrived(size, bulk_sem.at[stream], stream)
        if stream in (OWN_S, X_S, Y_S, D_S):
            moved.wait_recv()
        moved.wait_send()
    early_all.wait_send()
    put = gathered.at[0, pl.ds(0, late_rows), :]
    pltpu.make_async_copy(put, put, late_sem).wait()
    for which, box in enumerate((box_first, box_next, box_rest)):
        exchanged(box, which).wait_send()


def writes_of(parts, m, rows, me):
    p = len(parts) - 3 + m
    chunks = parts[p][3]
    height, half, late = rows // chunks, chunks // 2, late_pairs(parts, p)
    for d in range(8):
        owner = opposite(me, d)
        core = lax.rem(owner, 2)
        if late == 0 or d < 6:
            yield owner * rows, rows
        elif late == half:
            yield owner * rows + core * half * height, (half - 1) * height
        else:
            yield owner * rows + core * late * height, half * height
            yield owner * rows + (half + late) * height, (half - late) * height


def write_out(parts, gathered, targets, sems):
    rows = gathered.shape[1] // 8
    copies = []
    for m, target in targets:
        for at, size in writes_of(parts, m, rows, lax.axis_index("rows")):
            at = pl.multiple_of(at, 16)
            copies.append(
                pltpu.make_async_copy(
                    gathered.at[m, pl.ds(at, size), :], target.at[pl.ds(at, size), :], sems.at[len(copies)]
                )
            )
    for c in copies:
        c.start()
    return copies


def settle(parts, factors, gathered, query, key, *refs):
    copies = write_out(parts, gathered, ((0, query), (1, key)), refs[-1])
    for m in range(3):
        refs[m][...] = factors[m, 0]
    for c in copies:
        c.wait()


def settle_value(parts, gathered, key, out_key, value, sems):
    for c in write_out(parts, gathered, ((2, value),), sems):
        c.wait()


def finish(places, *refs):
    given = refs[:len(places)]
    key, value, sems = refs[-3:]
    rows = value.shape[0] // 8
    copies = []

    def write(ref, size, out, at):
        at = pl.multiple_of(at, 16)
        copies.append(pltpu.make_async_copy(ref, out.at[pl.ds(at, size), :], sems.at[len(copies)]))

    for ref, (matrix, d) in zip(given, places):
        owner = opposite(lax.axis_index("rows"), d)
        core, size = lax.rem(owner, 2), ref.shape[0]
        if matrix is None:
            write(ref, size, value, owner * rows + (1 + core) * (rows // 2) - size)
        else:
            write(ref, size, (key, value)[matrix - 1], owner * rows + (1 - core) * (rows // 2))
    for c in copies:
        c.start()
    for c in copies:
        c.wait()


def gathered_by_kernel(*arrays):
    rows, columns = arrays[0].shape
    parts = parts_of(columns)
    late_rows = [rows // part[3] * late_pairs(parts, p) for p, part in enumerate(parts)]
    vmem, hbm = pl.BlockSpec(memory_space=pltpu.VMEM), pl.BlockSpec(memory_space=pltpu.HBM)
    anywhere = pl.BlockSpec(memory_space=pl.ANY)
    dma = pltpu.SemaphoreType.DMA
    results = pl.pallas_call(
        functools.partial(kernel, parts),
        out_shape=[
            pltpu.VMEM((3, 1, columns), jnp.float32),
            pltpu.VMEM((3, 8 * rows, columns), jnp.bfloat16),
            pltpu.VMEM((late_rows[-2], columns), jnp.bfloat16),
            pltpu.VMEM((late_rows[-1], columns), jnp.bfloat16),
            pltpu.VMEM((rows // parts[-1][3], columns), jnp.bfloat16),
        ],
        in_specs=[hbm] * 8,
        out_specs=[vmem] * 5,
        scratch_shapes=[
            pltpu.VMEM((6, rows, columns), jnp.float32),
            pltpu.VMEM((rows,), jnp.float32),
            pltpu.VMEM((rows,), jnp.float32),
            pltpu.VMEM((rows, LANES), jnp.float32),
            pltpu.VMEM((rows, LANES), jnp.float32),
            pltpu.VMEM((8, 1, parts[0][2]), jnp.float32),
            pltpu.VMEM((8, 1, parts[1][2]), jnp.float32),
            pltpu.VMEM((8, 2, columns), jnp.float32),
            pltpu.VMEM((2, 2, rows // parts[0][3], parts[0][2]), jnp.float32),
            dma((4,)),
            dma((7,)),
            dma((7,)),
            dma((sum(part[3] for part in parts),)),
            dma((sum(part[3] // 2 for part in parts),)),
            dma((6,)),
            dma(()),
            dma((2,)),
            dma((2,)),
        ],
        compiler_params=pltpu.CompilerParams(
            collective_id=0, has_side_effects=True, vmem_limit_bytes=21 * 2**20
        ),
    )(*arrays)
    factors, gathered, late_key, late_value, closing = [
        pltpu.with_memory_space_constraint(r, pltpu.VMEM) for r in results
    ]
    whole = jax.ShapeDtypeStruct((8 * rows, columns), jnp.bfloat16)
    scales = jax.ShapeDtypeStruct((columns,), jnp.float32)
    limit = pltpu.CompilerParams(vmem_limit_bytes=2**20)

    def cost(size):
        return pl.CostEstimate(flops=0, bytes_accessed=size, transcendentals=0)

    across = [(i, i ^ (2, 4)[i % 2]) for i in range(8)]
    siblings = [(i, i ^ 1) for i in range(8)]
    value_mine = lax.ppermute(late_value, "rows", across)
    key_mine = lax.ppermute(late_key, "rows", across)
    closing_other = lax.ppermute(closing, "rows", siblings)
    query, key, *factors = pl.pallas_call(
        functools.partial(settle, parts),
        out_shape=[whole] * 2 + [scales] * 3,
        in_specs=[vmem] * 2,
        out_specs=[anywhere] * 2 + [vmem] * 3,
        scratch_shapes=[dma((18,))],
        cost_estimate=cost(32 * rows * columns),
        compiler_params=limit,
    )(factors, gathered)
    value_mine, closing_other, key = lax.optimization_barrier((value_mine, closing_other, key))
    value_other = lax.ppermute(value_mine, "rows", siblings)
    key, value = pl.pallas_call(
        functools.partial(settle_value, parts),
        out_shape=[whole] * 2,
        in_specs=[vmem, anywhere],
        out_specs=[anywhere] * 2,
        scratch_shapes=[dma((8,))],
        input_output_aliases={1: 0},
        cost_estimate=cost(16 * rows * columns),
        compiler_params=limit,
    )(gathered, key)
    key_mine, value_other, key, value = lax.optimization_barrier((key_mine, value_other, key, value))
    key_other = lax.ppermute(key_mine, "rows", siblings)
    for places, given in (
        (
            ((2, 6), (1, 6), (None, 6), (None, 7), (2, 7)),
            (value_mine, key_mine, closing, closing_other, value_other),
        ),
        (((1, 7),), (key_other,)),
    ):
        n = len(given)
        key, value = pl.pallas_call(
            functools.partial(finish, places),
            out_shape=[whole] * 2,
            in_specs=[vmem] * n + [anywhere] * 2,
            out_specs=[anywhere] * 2,
            scratch_shapes=[dma((n,))],
            input_output_aliases={n: 0, n + 1: 1},
            cost_estimate=cost(8 * late_rows[-1] * columns),
            compiler_params=limit,
        )(*given, key, value)
    return query, key, value, *factors


def solution(mesh):
    placed = (P("rows", "model"),) * 6 + (P("rows"),) * 2
    relayed = mesh.shape["rows"] == 8
    return jax.shard_map(
        gathered_by_kernel if relayed else gathered_by_collectives,
        mesh=mesh,
        in_specs=placed,
        out_specs=(P(None, "model"),) * 3 + (P("model"),) * 3,
        check_vma=False,
    )
```

```python
import functools

import jax
import jax.numpy as jnp
from jax import lax
from jax.experimental import pallas as pl
from jax.experimental.pallas import tpu as pltpu
from jax.sharding import PartitionSpec as P


MESH = pl.DeviceIdType.MESH
LANES = 128
OWN_X, OWN_Y, OWN_S, DIAG, X_S, Y_S, D_S = range(7)


def gathered_by_collectives(one_query, other_query, one_key, other_key, one_value, other_value, mix_share, norm_gain):
    share, gain = mix_share[:, None], norm_gain[:, None]
    gained = [
        (share * one + (1.0 - share) * other) * gain
        for one, other in ((one_query, other_query), (one_key, other_key), (one_value, other_value))
    ]
    factors = lax.pmax(tuple(jnp.max(jnp.abs(g), axis=0) for g in gained), "rows")
    narrow = [(g / f).astype(jnp.bfloat16) for g, f in zip(gained, factors)]
    return (*(lax.all_gather(w, "rows", axis=0, tiled=True) for w in narrow), *factors)


def opposite(me, d):
    core, east, north = lax.rem(me, 2), lax.rem(me // 2, 2), me // 4
    return (
        lax.rem(north + d // 4, 2) * 4
        + lax.rem(east + (d // 2) % 2, 2) * 2
        + lax.rem(core + d % 2, 2)
    )


def parts_of(columns):
    first = 2 * LANES
    return (
        (0, 0, first, 10),
        (0, first, columns - first, 2),
        (1, 0, columns, 10),
        (2, 0, columns, 10),
    )


def waits_of(parts):
    return tuple(
        (part[3], part[3] // 2) if p == 0 else (2 if part[3] > 2 else 1, 1)
        for p, part in enumerate(parts)
    )


def late_pairs(parts, p):
    return {len(parts) - 2: 3, len(parts) - 1: parts[p][3] // 2}.get(p, 0)


def kernel(parts, *refs):
    args, factors, gathered, late_key, late_value, closing = refs[0:8], *refs[8:13]
    (held, share, gain, wide_one, wide_other, box_first, box_next, box_rest, early,
     load_sem, send_sem, bulk_sem, own_sem, d_sem, box_sem, late_sem, early_sem, row_sem) = refs[13:]
    rows, columns = args[0].shape
    every = range(len(parts))
    late_rows = late_key.shape[0] + late_value.shape[0]
    waits = waits_of(parts)
    own_base = [sum(q[3] // w[0] for q, w in zip(parts[:p], waits)) for p in every]
    d_base = [sum(q[3] // 2 // w[1] for q, w in zip(parts[:p], waits)) for p in every]
    bulk = {OWN_S: 0, X_S: 1, Y_S: 2, D_S: 3}

    def own_arrival(p, k):
        return own_sem.at[own_base[p] + k // waits[p][0]]

    def d_arrival(p, j):
        return d_sem.at[d_base[p] + j // waits[p][1]]


    me = lax.axis_index("rows")
    core = lax.rem(me, 2)
    sibling, at_x, at_y, at_d = (opposite(me, d) for d in (1, 2, 4, 6))
    near = at_x + core * (at_y - at_x)
    side = at_y + core * (at_x - at_y)

    def columns_of(p):
        return pl.ds(parts[p][1], parts[p][2])

    def load(p):
        m = parts[p][0]
        for i in (2 * m, 2 * m + 1):
            pltpu.make_async_copy(
                args[i].at[:, columns_of(p)], held.at[i, :, columns_of(p)], load_sem.at[p]
            ).start()

    def loaded(p):
        ref = held.at[pl.ds(2 * parts[p][0], 2), :, columns_of(p)]
        pltpu.make_async_copy(ref, ref, load_sem.at[p]).wait()

    by_row = [pltpu.make_async_copy(args[6 + i], to, row_sem.at[i]) for i, to in enumerate((share, gain))]
    for c in by_row:
        c.start()
    load(0)

    barrier = pltpu.get_barrier_semaphore()
    for d in range(1, 8):
        pl.semaphore_signal(barrier, inc=1, device_id={"rows": opposite(me, d)}, device_id_type=MESH)

    for c in by_row:
        c.wait()
    for j in range(rows // LANES):
        s = jnp.broadcast_to(share[j * LANES:(j + 1) * LANES][None], (LANES, LANES)).T
        g = jnp.broadcast_to(gain[j * LANES:(j + 1) * LANES][None], (LANES, LANES)).T
        wide_one[j * LANES:(j + 1) * LANES, :] = s * g
        wide_other[j * LANES:(j + 1) * LANES, :] = (1.0 - s) * g

    def mix(p):
        m, _, width, _ = parts[p]

        def body(i, top):
            at = pl.ds(pl.multiple_of(i * 8, 8), 8)
            a = jnp.concatenate([wide_one[at, :]] * (width // LANES), axis=1)
            b = jnp.concatenate([wide_other[at, :]] * (width // LANES), axis=1)
            mixed = a * held[2 * m, at, columns_of(p)] + b * held[2 * m + 1, at, columns_of(p)]
            held[2 * m, at, columns_of(p)] = mixed
            return jnp.maximum(top, jnp.abs(mixed))

        top = lax.fori_loop(0, rows // 8, body, jnp.zeros((8, width), jnp.float32), unroll=4)
        return jnp.max(top, axis=0, keepdims=True)

    def exchange(box, which):
        for d in (6, 7, 2, 4, 3, 5, 1):
            pltpu.make_async_remote_copy(
                box.at[me], box.at[me], box_sem.at[2 * which], box_sem.at[2 * which + 1],
                device_id={"rows": opposite(me, d)}, device_id_type=MESH,
            ).start()

    def exchanged(box, which):
        return pltpu.make_async_remote_copy(
            box.at[pl.ds(0, 7)], box.at[pl.ds(0, 7)], box_sem.at[2 * which], box_sem.at[2 * which + 1],
            device_id={"rows": sibling}, device_id_type=MESH,
        )

    def height(p):
        return rows // parts[p][3]

    def piece(p, owner, k, count=1):
        at = pl.multiple_of(owner * rows + k * height(p), 16)
        return gathered.at[parts[p][0], pl.ds(at, count * height(p)), columns_of(p)]

    def send(p, owner, k, stream, target, arrive, to=None):
        ref = piece(p, owner, k)
        pltpu.make_async_remote_copy(
            ref, ref if to is None else to, send_sem.at[stream], arrive,
            device_id={"rows": target}, device_id_type=MESH,
        ).start()

    def arrived(ref, arrive, stream=0):
        return pltpu.make_async_remote_copy(
            ref, ref, send_sem.at[stream], arrive, device_id={"rows": sibling}, device_id_type=MESH
        )

    def narrow(p, k, inverse):
        m = parts[p][0]

        def body(i, _):
            at = pl.multiple_of(k * height(p) + i * 16, 16)
            small = (held[2 * m, pl.ds(at, 16), columns_of(p)] * inverse).astype(jnp.bfloat16)
            gathered[m, pl.ds(pl.multiple_of(me * rows + at, 16), 16), columns_of(p)] = small
            return 0

        lax.fori_loop(0, height(p) // 16, body, 0, unroll=True)

    def send_own(p, k):
        if p or k not in ahead:
            send(p, me, k, OWN_X, at_x, own_arrival(p, k))
            send(p, me, k, OWN_Y, at_y, own_arrival(p, k))
        send(p, me, k, OWN_S, sibling, bulk_sem.at[bulk[OWN_S]])

    def narrow_and_send(p, factor, sent):
        factors[parts[p][0], :, columns_of(p)] = factor
        inverse = 1.0 / factor
        for k in range(parts[p][3]):
            narrow(p, k, inverse)
            if 1 <= k <= sent:
                send_own(p, k - 1)
        if sent == parts[p][3]:
            send_own(p, sent - 1)

    ahead = (0, parts[0][3] // 2)

    def send_early():
        for place, target in enumerate((at_x, at_y)):
            for i, k in enumerate(ahead):
                pltpu.make_async_remote_copy(
                    held.at[0, pl.ds(k * height(0), height(0)), columns_of(0)],
                    early.at[place, i],
                    early_sem.at[0],
                    early_sem.at[1],
                    device_id={"rows": target},
                    device_id_type=MESH,
                ).start()

    early_all = pltpu.make_async_remote_copy(
        early, early, early_sem.at[0], early_sem.at[1], device_id={"rows": at_x}, device_id_type=MESH
    )

    def narrow_early():
        early_all.wait_recv()
        inverse = 1.0 / factors[0, :, columns_of(0)]
        for place, owner in enumerate((at_x, at_y)):
            for i, k in enumerate(ahead):
                for r in range(0, height(0), 16):
                    at = pl.multiple_of(owner * rows + k * height(0) + r, 16)
                    small = (early[place, i, r:r + 16, :] * inverse).astype(jnp.bfloat16)
                    gathered[0, pl.ds(at, 16), columns_of(0)] = small

    loaded(0)
    load(1)
    box_first[me] = mix(0)
    pl.semaphore_wait(barrier, 7)
    exchange(box_first, 0)
    send_early()
    exchanged(box_first, 0).wait_recv()
    narrow_and_send(0, jnp.max(box_first[...], axis=0), 3)
    loaded(1)
    load(2)
    load(3)
    box_next[me] = mix(1)
    exchange(box_next, 1)
    for k in range(3, parts[0][3]):
        send_own(0, k)
    narrow_early()
    exchanged(box_next, 1).wait_recv()
    narrow_and_send(1, jnp.max(box_next[...], axis=0), parts[1][3] // 2)
    loaded(2)
    box_rest[me, 0:1] = mix(2)
    loaded(3)
    box_rest[me, 1:2] = mix(3)
    exchange(box_rest, 2)
    for k in range(parts[1][3] // 2, parts[1][3]):
        send_own(1, k)
    exchanged(box_rest, 2).wait_recv()
    both = jnp.max(box_rest[...], axis=0)
    for p in (2, 3):
        narrow_and_send(p, both[p - 2:p - 1], parts[p][3])

    def closes(p, j):
        return p == every[-1] and j == parts[p][3] // 2 - 1

    for p in every:
        chunks = parts[p][3]
        half = chunks // 2
        for k in range(chunks):
            if k % waits[p][0] == 0:
                count = waits[p][0] - (0 if p else len(ahead))
                arrived(piece(p, 0, 0, 2 * count), own_arrival(p, k)).wait_recv()
            send(p, at_x, k, X_S, sibling, bulk_sem.at[bulk[X_S]])
            send(p, at_y, k, Y_S, sibling, bulk_sem.at[bulk[Y_S]])
            j = k % half
            if j >= late_pairs(parts, p):
                if k < half:
                    send(p, at_x, k, DIAG, at_y, d_arrival(p, j))
                else:
                    send(p, at_y, k, DIAG, at_x, d_arrival(p, j))
            elif k >= half:
                send(
                    p, near, j + core * half, DIAG, side, d_arrival(p, j),
                    closing if closes(p, j) else None,
                )
                pltpu.make_async_copy(
                    piece(p, side, j + (1 - core) * half),
                    (late_value if p == every[-1] else late_key).at[pl.ds(j * height(p), height(p)), :],
                    late_sem,
                ).start()
    for p in every:
        half = parts[p][3] // 2
        for j in range(half):
            if j >= late_pairs(parts, p):
                if j % waits[p][1] == 0:
                    arrived(piece(p, 0, 0, 2 * waits[p][1]), d_arrival(p, j)).wait_recv()
                send(p, at_d, j, D_S, sibling, bulk_sem.at[bulk[D_S]])
                send(p, at_d, j + half, D_S, sibling, bulk_sem.at[bulk[D_S]])
            else:
                arrived(piece(p, 0, 0, 1), d_arrival(p, j)).wait_recv()
                if not closes(p, j):
                    send(p, at_d, j + core * half, D_S, sibling, bulk_sem.at[bulk[D_S]])

    width = parts[0][2]
    sizes = {
        stream: gathered.at[:, pl.ds(0, rows), :] for stream in (OWN_S, X_S, Y_S)
    } | {
        DIAG: gathered.at[0, pl.ds(0, 3 * rows - late_rows), :],
        D_S: gathered.at[0, pl.ds(0, 3 * rows - late_rows - closing.shape[0]), :],
    } | {
        stream: gathered.at[pl.ds(0, 2), pl.ds(0, 3 * rows * columns // (2 * width) - height(0)), pl.ds(0, width)]
        for stream in (OWN_X, OWN_Y)
    }
    for stream, size in sizes.items():
        moved = arrived(size, bulk_sem.at[bulk.get(stream, 0)], stream)
        if stream in bulk:
            moved.wait_recv()
        moved.wait_send()
    early_all.wait_send()
    put = gathered.at[0, pl.ds(0, late_rows), :]
    pltpu.make_async_copy(put, put, late_sem).wait()
    for which, box in enumerate((box_first, box_next, box_rest)):
        exchanged(box, which).wait_send()


def writes_of(parts, m, rows, me):
    p = len(parts) - 3 + m
    chunks = parts[p][3]
    height, half, late = rows // chunks, chunks // 2, late_pairs(parts, p)
    for d in range(8):
        owner = opposite(me, d)
        core = lax.rem(owner, 2)
        if late == 0 or d < 6:
            yield owner * rows, rows
        elif late == half:
            yield owner * rows + core * half * height, (half - 1) * height
        else:
            yield owner * rows + core * late * height, half * height
            yield owner * rows + (half + late) * height, (half - late) * height


def write_out(parts, gathered, targets, sems):
    rows = gathered.shape[1] // 8
    copies = []
    for m, target in targets:
        for at, size in writes_of(parts, m, rows, lax.axis_index("rows")):
            at = pl.multiple_of(at, 16)
            copies.append(
                pltpu.make_async_copy(
                    gathered.at[m, pl.ds(at, size), :], target.at[pl.ds(at, size), :], sems.at[len(copies)]
                )
            )
    for c in copies:
        c.start()
    return copies


def settle(parts, factors, gathered, query, key, *refs):
    copies = write_out(parts, gathered, ((0, query), (1, key)), refs[-1])
    for m in range(3):
        refs[m][...] = factors[m, 0]
    for c in copies:
        c.wait()


def settle_value(parts, gathered, key, out_key, value, sems):
    for c in write_out(parts, gathered, ((2, value),), sems):
        c.wait()


def finish(places, *refs):
    given = refs[:len(places)]
    key, value, sems = refs[-3:]
    rows = value.shape[0] // 8
    copies = []

    def write(ref, size, out, at):
        at = pl.multiple_of(at, 16)
        copies.append(pltpu.make_async_copy(ref, out.at[pl.ds(at, size), :], sems.at[len(copies)]))

    for ref, (matrix, d) in zip(given, places):
        owner = opposite(lax.axis_index("rows"), d)
        core, size = lax.rem(owner, 2), ref.shape[0]
        if matrix is None:
            write(ref, size, value, owner * rows + (1 + core) * (rows // 2) - size)
        else:
            write(ref, size, (key, value)[matrix - 1], owner * rows + (1 - core) * (rows // 2))
    for c in copies:
        c.start()
    for c in copies:
        c.wait()


def gathered_by_kernel(*arrays):
    rows, columns = arrays[0].shape
    parts = parts_of(columns)
    waits = waits_of(parts)
    late_rows = [rows // part[3] * late_pairs(parts, p) for p, part in enumerate(parts)]
    vmem, hbm = pl.BlockSpec(memory_space=pltpu.VMEM), pl.BlockSpec(memory_space=pltpu.HBM)
    anywhere = pl.BlockSpec(memory_space=pl.ANY)
    dma = pltpu.SemaphoreType.DMA
    results = pl.pallas_call(
        functools.partial(kernel, parts),
        out_shape=[
            pltpu.VMEM((3, 1, columns), jnp.float32),
            pltpu.VMEM((3, 8 * rows, columns), jnp.bfloat16),
            pltpu.VMEM((late_rows[-2], columns), jnp.bfloat16),
            pltpu.VMEM((late_rows[-1], columns), jnp.bfloat16),
            pltpu.VMEM((rows // parts[-1][3], columns), jnp.bfloat16),
        ],
        in_specs=[hbm] * 8,
        out_specs=[vmem] * 5,
        scratch_shapes=[
            pltpu.VMEM((6, rows, columns), jnp.float32),
            pltpu.VMEM((rows,), jnp.float32),
            pltpu.VMEM((rows,), jnp.float32),
            pltpu.VMEM((rows, LANES), jnp.float32),
            pltpu.VMEM((rows, LANES), jnp.float32),
            pltpu.VMEM((8, 1, parts[0][2]), jnp.float32),
            pltpu.VMEM((8, 1, parts[1][2]), jnp.float32),
            pltpu.VMEM((8, 2, columns), jnp.float32),
            pltpu.VMEM((2, 2, rows // parts[0][3], parts[0][2]), jnp.float32),
            dma((4,)),
            dma((7,)),
            dma((4,)),
            dma((sum(part[3] // w[0] for part, w in zip(parts, waits)),)),
            dma((sum(part[3] // 2 // w[1] for part, w in zip(parts, waits)),)),
            dma((6,)),
            dma(()),
            dma((2,)),
            dma((2,)),
        ],
        compiler_params=pltpu.CompilerParams(
            collective_id=0, has_side_effects=True, vmem_limit_bytes=21 * 2**20
        ),
    )(*arrays)
    factors, gathered, late_key, late_value, closing = [
        pltpu.with_memory_space_constraint(r, pltpu.VMEM) for r in results
    ]
    whole = jax.ShapeDtypeStruct((8 * rows, columns), jnp.bfloat16)
    scales = jax.ShapeDtypeStruct((columns,), jnp.float32)
    limit = pltpu.CompilerParams(vmem_limit_bytes=2**20)

    def cost(size):
        return pl.CostEstimate(flops=0, bytes_accessed=size, transcendentals=0)

    across = [(i, i ^ (2, 4)[i % 2]) for i in range(8)]
    siblings = [(i, i ^ 1) for i in range(8)]
    value_mine = lax.ppermute(late_value, "rows", across)
    key_mine = lax.ppermute(late_key, "rows", across)
    closing_other = lax.ppermute(closing, "rows", siblings)
    query, key, *factors = pl.pallas_call(
        functools.partial(settle, parts),
        out_shape=[whole] * 2 + [scales] * 3,
        in_specs=[vmem] * 2,
        out_specs=[anywhere] * 2 + [vmem] * 3,
        scratch_shapes=[dma((18,))],
        cost_estimate=cost(32 * rows * columns),
        compiler_params=limit,
    )(factors, gathered)
    value_mine, closing_other, key = lax.optimization_barrier((value_mine, closing_other, key))
    value_other = lax.ppermute(value_mine, "rows", siblings)
    key, value = pl.pallas_call(
        functools.partial(settle_value, parts),
        out_shape=[whole] * 2,
        in_specs=[vmem, anywhere],
        out_specs=[anywhere] * 2,
        scratch_shapes=[dma((8,))],
        input_output_aliases={1: 0},
        cost_estimate=cost(16 * rows * columns),
        compiler_params=limit,
    )(gathered, key)
    key_mine, value_other, key, value = lax.optimization_barrier((key_mine, value_other, key, value))
    key_other = lax.ppermute(key_mine, "rows", siblings)
    for places, given in (
        (
            ((2, 6), (1, 6), (None, 6), (None, 7), (2, 7)),
            (value_mine, key_mine, closing, closing_other, value_other),
        ),
        (((1, 7),), (key_other,)),
    ):
        n = len(given)
        key, value = pl.pallas_call(
            functools.partial(finish, places),
            out_shape=[whole] * 2,
            in_specs=[vmem] * n + [anywhere] * 2,
            out_specs=[anywhere] * 2,
            scratch_shapes=[dma((n,))],
            input_output_aliases={n: 0, n + 1: 1},
            cost_estimate=cost(8 * late_rows[-1] * columns),
            compiler_params=limit,
        )(*given, key, value)
    return query, key, value, *factors


def solution(mesh):
    placed = (P("rows", "model"),) * 6 + (P("rows"),) * 2
    relayed = mesh.shape["rows"] == 8
    return jax.shard_map(
        gathered_by_kernel if relayed else gathered_by_collectives,
        mesh=mesh,
        in_specs=placed,
        out_specs=(P(None, "model"),) * 3 + (P("model"),) * 3,
        check_vma=False,
    )
```

```python
import functools

import jax
import jax.numpy as jnp
from jax import lax
from jax.experimental import pallas as pl
from jax.experimental.pallas import tpu as pltpu
from jax.sharding import PartitionSpec as P


MESH = pl.DeviceIdType.MESH
LANES = 128
OWN_X, OWN_Y, OWN_S, DIAG, X_S, Y_S, D_S = range(7)


def gathered_by_collectives(one_query, other_query, one_key, other_key, one_value, other_value, mix_share, norm_gain):
    share, gain = mix_share[:, None], norm_gain[:, None]
    gained = [
        (share * one + (1.0 - share) * other) * gain
        for one, other in ((one_query, other_query), (one_key, other_key), (one_value, other_value))
    ]
    factors = lax.pmax(tuple(jnp.max(jnp.abs(g), axis=0) for g in gained), "rows")
    narrow = [(g / f).astype(jnp.bfloat16) for g, f in zip(gained, factors)]
    return (*(lax.all_gather(w, "rows", axis=0, tiled=True) for w in narrow), *factors)


def opposite(me, d):
    core, east, north = lax.rem(me, 2), lax.rem(me // 2, 2), me // 4
    return (
        lax.rem(north + d // 4, 2) * 4
        + lax.rem(east + (d // 2) % 2, 2) * 2
        + lax.rem(core + d % 2, 2)
    )


def parts_of(columns):
    first = 2 * LANES
    return (
        (0, 0, first, 10),
        (0, first, columns - first, 2),
        (1, 0, columns, 10),
        (2, 0, columns, 10),
    )


def waits_of(parts):
    return tuple(
        (part[3], part[3] // 2) if p == 0 else (2 if part[3] > 2 else 1, 1)
        for p, part in enumerate(parts)
    )


def late_pairs(parts, p):
    return {len(parts) - 2: 3, len(parts) - 1: parts[p][3] // 2}.get(p, 0)


def kernel(parts, *refs):
    args, factors, gathered, late_key, late_value, closing = refs[0:8], *refs[8:13]
    (held, share, gain, wide_one, wide_other, box_first, box_next, box_rest, early,
     load_sem, send_sem, bulk_sem, own_sem, d_sem, box_sem, late_sem, early_sem, row_sem) = refs[13:]
    rows, columns = args[0].shape
    every = range(len(parts))
    late_rows = late_key.shape[0] + late_value.shape[0]
    waits = waits_of(parts)
    own_base = [sum(q[3] // w[0] for q, w in zip(parts[:p], waits)) for p in every]
    d_base = [sum(q[3] // 2 // w[1] for q, w in zip(parts[:p], waits)) for p in every]
    bulk = {OWN_S: 0, X_S: 1, Y_S: 2, D_S: 3}

    def own_arrival(p, k):
        return own_sem.at[own_base[p] + k // waits[p][0]]

    def d_arrival(p, j):
        return d_sem.at[d_base[p] + j // waits[p][1]]


    me = lax.axis_index("rows")
    core = lax.rem(me, 2)
    sibling, at_x, at_y, at_d = (opposite(me, d) for d in (1, 2, 4, 6))
    near = at_x + core * (at_y - at_x)
    side = at_y + core * (at_x - at_y)

    def columns_of(p):
        return pl.ds(parts[p][1], parts[p][2])

    def load(p):
        m = parts[p][0]
        cuts = 1 if p else 5
        for cut in range(cuts):
            at = pl.ds(cut * (rows // cuts), rows // cuts)
            for i in (2 * m, 2 * m + 1):
                pltpu.make_async_copy(
                    args[i].at[at, columns_of(p)], held.at[i, at, columns_of(p)], load_sem.at[p]
                ).start()

    def loaded(p):
        ref = held.at[pl.ds(2 * parts[p][0], 2), :, columns_of(p)]
        pltpu.make_async_copy(ref, ref, load_sem.at[p]).wait()

    load(0)
    by_row = [pltpu.make_async_copy(args[6 + i], to, row_sem.at[i]) for i, to in enumerate((share, gain))]
    for c in by_row:
        c.start()

    barrier = pltpu.get_barrier_semaphore()
    for d in range(1, 8):
        pl.semaphore_signal(barrier, inc=1, device_id={"rows": opposite(me, d)}, device_id_type=MESH)

    for c in by_row:
        c.wait()
    for j in range(rows // LANES):
        s = jnp.broadcast_to(share[j * LANES:(j + 1) * LANES][None], (LANES, LANES)).T
        g = jnp.broadcast_to(gain[j * LANES:(j + 1) * LANES][None], (LANES, LANES)).T
        wide_one[j * LANES:(j + 1) * LANES, :] = s * g
        wide_other[j * LANES:(j + 1) * LANES, :] = (1.0 - s) * g

    def mix(p):
        m, _, width, _ = parts[p]

        def body(i, top):
            at = pl.ds(pl.multiple_of(i * 8, 8), 8)
            a = jnp.concatenate([wide_one[at, :]] * (width // LANES), axis=1)
            b = jnp.concatenate([wide_other[at, :]] * (width // LANES), axis=1)
            mixed = a * held[2 * m, at, columns_of(p)] + b * held[2 * m + 1, at, columns_of(p)]
            held[2 * m, at, columns_of(p)] = mixed
            return jnp.maximum(top, jnp.abs(mixed))

        top = lax.fori_loop(0, rows // 8, body, jnp.zeros((8, width), jnp.float32), unroll=4 if p else 16)
        return jnp.max(top, axis=0, keepdims=True)

    def exchange(box, which):
        for d in (6, 7, 2, 4, 3, 5, 1):
            pltpu.make_async_remote_copy(
                box.at[me], box.at[me], box_sem.at[2 * which], box_sem.at[2 * which + 1],
                device_id={"rows": opposite(me, d)}, device_id_type=MESH,
            ).start()

    def exchanged(box, which):
        return pltpu.make_async_remote_copy(
            box.at[pl.ds(0, 7)], box.at[pl.ds(0, 7)], box_sem.at[2 * which], box_sem.at[2 * which + 1],
            device_id={"rows": sibling}, device_id_type=MESH,
        )

    def height(p):
        return rows // parts[p][3]

    def piece(p, owner, k, count=1):
        at = pl.multiple_of(owner * rows + k * height(p), 16)
        return gathered.at[parts[p][0], pl.ds(at, count * height(p)), columns_of(p)]

    def send(p, owner, k, stream, target, arrive, to=None):
        ref = piece(p, owner, k)
        pltpu.make_async_remote_copy(
            ref, ref if to is None else to, send_sem.at[stream], arrive,
            device_id={"rows": target}, device_id_type=MESH,
        ).start()

    def arrived(ref, arrive, stream=0):
        return pltpu.make_async_remote_copy(
            ref, ref, send_sem.at[stream], arrive, device_id={"rows": sibling}, device_id_type=MESH
        )

    def narrow(p, k, inverse):
        m = parts[p][0]

        def body(i, _):
            at = pl.multiple_of(k * height(p) + i * 16, 16)
            small = (held[2 * m, pl.ds(at, 16), columns_of(p)] * inverse).astype(jnp.bfloat16)
            gathered[m, pl.ds(pl.multiple_of(me * rows + at, 16), 16), columns_of(p)] = small
            return 0

        lax.fori_loop(0, height(p) // 16, body, 0, unroll=True)

    def send_own(p, k):
        if p or k not in ahead:
            send(p, me, k, OWN_X, at_x, own_arrival(p, k))
            send(p, me, k, OWN_Y, at_y, own_arrival(p, k))
        send(p, me, k, OWN_S, sibling, bulk_sem.at[bulk[OWN_S]])

    def narrow_and_send(p, factor, sent):
        factors[parts[p][0], :, columns_of(p)] = factor
        inverse = 1.0 / factor
        for k in range(parts[p][3]):
            narrow(p, k, inverse)
            if 1 <= k <= sent:
                send_own(p, k - 1)
        if sent == parts[p][3]:
            send_own(p, sent - 1)

    ahead = (0, parts[0][3] // 2)

    def send_early():
        for place, target in enumerate((at_x, at_y)):
            for i, k in enumerate(ahead):
                pltpu.make_async_remote_copy(
                    held.at[0, pl.ds(k * height(0), height(0)), columns_of(0)],
                    early.at[place, i],
                    early_sem.at[0],
                    early_sem.at[1],
                    device_id={"rows": target},
                    device_id_type=MESH,
                ).start()

    early_all = pltpu.make_async_remote_copy(
        early, early, early_sem.at[0], early_sem.at[1], device_id={"rows": at_x}, device_id_type=MESH
    )

    def narrow_early():
        early_all.wait_recv()
        inverse = 1.0 / factors[0, :, columns_of(0)]
        for place, owner in enumerate((at_x, at_y)):
            for i, k in enumerate(ahead):
                for r in range(0, height(0), 16):
                    at = pl.multiple_of(owner * rows + k * height(0) + r, 16)
                    small = (early[place, i, r:r + 16, :] * inverse).astype(jnp.bfloat16)
                    gathered[0, pl.ds(at, 16), columns_of(0)] = small

    loaded(0)
    load(1)
    box_first[me] = mix(0)
    pl.semaphore_wait(barrier, 7)
    exchange(box_first, 0)
    send_early()
    exchanged(box_first, 0).wait_recv()
    narrow_and_send(0, jnp.max(box_first[...], axis=0), 3)
    loaded(1)
    load(2)
    load(3)
    box_next[me] = mix(1)
    exchange(box_next, 1)
    for k in range(3, parts[0][3]):
        send_own(0, k)
    narrow_early()
    exchanged(box_next, 1).wait_recv()
    narrow_and_send(1, jnp.max(box_next[...], axis=0), parts[1][3] // 2)
    loaded(2)
    box_rest[me, 0:1] = mix(2)
    loaded(3)
    box_rest[me, 1:2] = mix(3)
    exchange(box_rest, 2)
    for k in range(parts[1][3] // 2, parts[1][3]):
        send_own(1, k)
    exchanged(box_rest, 2).wait_recv()
    both = jnp.max(box_rest[...], axis=0)
    for p in (2, 3):
        narrow_and_send(p, both[p - 2:p - 1], parts[p][3])

    def closes(p, j):
        return p == every[-1] and j == parts[p][3] // 2 - 1

    for p in every:
        chunks = parts[p][3]
        half = chunks // 2
        for k in range(chunks):
            if k % waits[p][0] == 0:
                count = waits[p][0] - (0 if p else len(ahead))
                arrived(piece(p, 0, 0, 2 * count), own_arrival(p, k)).wait_recv()
            send(p, at_x, k, X_S, sibling, bulk_sem.at[bulk[X_S]])
            send(p, at_y, k, Y_S, sibling, bulk_sem.at[bulk[Y_S]])
            j = k % half
            if j >= late_pairs(parts, p):
                if k < half:
                    send(p, at_x, k, DIAG, at_y, d_arrival(p, j))
                else:
                    send(p, at_y, k, DIAG, at_x, d_arrival(p, j))
            elif k >= half:
                send(
                    p, near, j + core * half, DIAG, side, d_arrival(p, j),
                    closing if closes(p, j) else None,
                )
                pltpu.make_async_copy(
                    piece(p, side, j + (1 - core) * half),
                    (late_value if p == every[-1] else late_key).at[pl.ds(j * height(p), height(p)), :],
                    late_sem,
                ).start()
    for p in every:
        half = parts[p][3] // 2
        for j in range(half):
            if j >= late_pairs(parts, p):
                if j % waits[p][1] == 0:
                    arrived(piece(p, 0, 0, 2 * waits[p][1]), d_arrival(p, j)).wait_recv()
                send(p, at_d, j, D_S, sibling, bulk_sem.at[bulk[D_S]])
                send(p, at_d, j + half, D_S, sibling, bulk_sem.at[bulk[D_S]])
            else:
                arrived(piece(p, 0, 0, 1), d_arrival(p, j)).wait_recv()
                if not closes(p, j):
                    send(p, at_d, j + core * half, D_S, sibling, bulk_sem.at[bulk[D_S]])

    width = parts[0][2]
    sizes = {
        stream: gathered.at[:, pl.ds(0, rows), :] for stream in (OWN_S, X_S, Y_S)
    } | {
        DIAG: gathered.at[0, pl.ds(0, 3 * rows - late_rows), :],
        D_S: gathered.at[0, pl.ds(0, 3 * rows - late_rows - closing.shape[0]), :],
    } | {
        stream: gathered.at[pl.ds(0, 2), pl.ds(0, 3 * rows * columns // (2 * width) - height(0)), pl.ds(0, width)]
        for stream in (OWN_X, OWN_Y)
    }
    for stream, size in sizes.items():
        moved = arrived(size, bulk_sem.at[bulk.get(stream, 0)], stream)
        if stream in bulk:
            moved.wait_recv()
        moved.wait_send()
    early_all.wait_send()
    put = gathered.at[0, pl.ds(0, late_rows), :]
    pltpu.make_async_copy(put, put, late_sem).wait()
    for which, box in enumerate((box_first, box_next, box_rest)):
        exchanged(box, which).wait_send()


def writes_of(parts, m, rows, me):
    p = len(parts) - 3 + m
    chunks = parts[p][3]
    height, half, late = rows // chunks, chunks // 2, late_pairs(parts, p)
    for d in range(8):
        owner = opposite(me, d)
        core = lax.rem(owner, 2)
        if late == 0 or d < 6:
            yield owner * rows, rows
        elif late == half:
            yield owner * rows + core * half * height, (half - 1) * height
        else:
            yield owner * rows + core * late * height, half * height
            yield owner * rows + (half + late) * height, (half - late) * height


def write_out(parts, gathered, targets, sems):
    rows = gathered.shape[1] // 8
    copies = []
    for m, target in targets:
        for at, size in writes_of(parts, m, rows, lax.axis_index("rows")):
            at = pl.multiple_of(at, 16)
            copies.append(
                pltpu.make_async_copy(
                    gathered.at[m, pl.ds(at, size), :], target.at[pl.ds(at, size), :], sems.at[len(copies)]
                )
            )
    for c in copies:
        c.start()
    return copies


def settle(parts, factors, gathered, query, key, *refs):
    copies = write_out(parts, gathered, ((0, query), (1, key)), refs[-1])
    for m in range(3):
        refs[m][...] = factors[m, 0]
    for c in copies:
        c.wait()


def settle_value(parts, gathered, key, out_key, value, sems):
    for c in write_out(parts, gathered, ((2, value),), sems):
        c.wait()


def finish(places, *refs):
    given = refs[:len(places)]
    key, value, sems = refs[-3:]
    rows = value.shape[0] // 8
    copies = []

    def write(ref, size, out, at):
        at = pl.multiple_of(at, 16)
        copies.append(pltpu.make_async_copy(ref, out.at[pl.ds(at, size), :], sems.at[len(copies)]))

    for ref, (matrix, d) in zip(given, places):
        owner = opposite(lax.axis_index("rows"), d)
        core, size = lax.rem(owner, 2), ref.shape[0]
        if matrix is None:
            write(ref, size, value, owner * rows + (1 + core) * (rows // 2) - size)
        else:
            write(ref, size, (key, value)[matrix - 1], owner * rows + (1 - core) * (rows // 2))
    for c in copies:
        c.start()
    for c in copies:
        c.wait()


def gathered_by_kernel(*arrays):
    rows, columns = arrays[0].shape
    parts = parts_of(columns)
    waits = waits_of(parts)
    late_rows = [rows // part[3] * late_pairs(parts, p) for p, part in enumerate(parts)]
    vmem, hbm = pl.BlockSpec(memory_space=pltpu.VMEM), pl.BlockSpec(memory_space=pltpu.HBM)
    anywhere = pl.BlockSpec(memory_space=pl.ANY)
    dma = pltpu.SemaphoreType.DMA
    results = pl.pallas_call(
        functools.partial(kernel, parts),
        out_shape=[
            pltpu.VMEM((3, 1, columns), jnp.float32),
            pltpu.VMEM((3, 8 * rows, columns), jnp.bfloat16),
            pltpu.VMEM((late_rows[-2], columns), jnp.bfloat16),
            pltpu.VMEM((late_rows[-1], columns), jnp.bfloat16),
            pltpu.VMEM((rows // parts[-1][3], columns), jnp.bfloat16),
        ],
        in_specs=[hbm] * 8,
        out_specs=[vmem] * 5,
        scratch_shapes=[
            pltpu.VMEM((6, rows, columns), jnp.float32),
            pltpu.VMEM((rows,), jnp.float32),
            pltpu.VMEM((rows,), jnp.float32),
            pltpu.VMEM((rows, LANES), jnp.float32),
            pltpu.VMEM((rows, LANES), jnp.float32),
            pltpu.VMEM((8, 1, parts[0][2]), jnp.float32),
            pltpu.VMEM((8, 1, parts[1][2]), jnp.float32),
            pltpu.VMEM((8, 2, columns), jnp.float32),
            pltpu.VMEM((2, 2, rows // parts[0][3], parts[0][2]), jnp.float32),
            dma((4,)),
            dma((7,)),
            dma((4,)),
            dma((sum(part[3] // w[0] for part, w in zip(parts, waits)),)),
            dma((sum(part[3] // 2 // w[1] for part, w in zip(parts, waits)),)),
            dma((6,)),
            dma(()),
            dma((2,)),
            dma((2,)),
        ],
        compiler_params=pltpu.CompilerParams(
            collective_id=0, has_side_effects=True, vmem_limit_bytes=21 * 2**20
        ),
    )(*arrays)
    factors, gathered, late_key, late_value, closing = [
        pltpu.with_memory_space_constraint(r, pltpu.VMEM) for r in results
    ]
    whole = jax.ShapeDtypeStruct((8 * rows, columns), jnp.bfloat16)
    scales = jax.ShapeDtypeStruct((columns,), jnp.float32)
    limit = pltpu.CompilerParams(vmem_limit_bytes=2**20)

    def cost(size):
        return pl.CostEstimate(flops=0, bytes_accessed=size, transcendentals=0)

    across = [(i, i ^ (2, 4)[i % 2]) for i in range(8)]
    siblings = [(i, i ^ 1) for i in range(8)]
    value_mine = lax.ppermute(late_value, "rows", across)
    key_mine = lax.ppermute(late_key, "rows", across)
    closing_other = lax.ppermute(closing, "rows", siblings)
    query, key, *factors = pl.pallas_call(
        functools.partial(settle, parts),
        out_shape=[whole] * 2 + [scales] * 3,
        in_specs=[vmem] * 2,
        out_specs=[anywhere] * 2 + [vmem] * 3,
        scratch_shapes=[dma((18,))],
        cost_estimate=cost(32 * rows * columns),
        compiler_params=limit,
    )(factors, gathered)
    value_mine, closing_other, key = lax.optimization_barrier((value_mine, closing_other, key))
    value_other = lax.ppermute(value_mine, "rows", siblings)
    key, value = pl.pallas_call(
        functools.partial(settle_value, parts),
        out_shape=[whole] * 2,
        in_specs=[vmem, anywhere],
        out_specs=[anywhere] * 2,
        scratch_shapes=[dma((8,))],
        input_output_aliases={1: 0},
        cost_estimate=cost(16 * rows * columns),
        compiler_params=limit,
    )(gathered, key)
    key_mine, value_other, key, value = lax.optimization_barrier((key_mine, value_other, key, value))
    key_other = lax.ppermute(key_mine, "rows", siblings)
    for places, given in (
        (
            ((2, 6), (1, 6), (None, 6), (None, 7), (2, 7)),
            (value_mine, key_mine, closing, closing_other, value_other),
        ),
        (((1, 7),), (key_other,)),
    ):
        n = len(given)
        key, value = pl.pallas_call(
            functools.partial(finish, places),
            out_shape=[whole] * 2,
            in_specs=[vmem] * n + [anywhere] * 2,
            out_specs=[anywhere] * 2,
            scratch_shapes=[dma((n,))],
            input_output_aliases={n: 0, n + 1: 1},
            cost_estimate=cost(8 * late_rows[-1] * columns),
            compiler_params=limit,
        )(*given, key, value)
    return query, key, value, *factors


def solution(mesh):
    placed = (P("rows", "model"),) * 6 + (P("rows"),) * 2
    relayed = mesh.shape["rows"] == 8
    return jax.shard_map(
        gathered_by_kernel if relayed else gathered_by_collectives,
        mesh=mesh,
        in_specs=placed,
        out_specs=(P(None, "model"),) * 3 + (P("model"),) * 3,
        check_vma=False,
    )
```
